32 devices in a mesh: dp: 1 (over z), ep: 32 (over y, x, core).
Axes of the slice: x: 4, y: 4, z: 1, core: 2. Of those that a mesh axis runs over, the one named last changes fastest.
The devices are a block of a 4x4x8 slice.
Arguments:
- tokens: bfloat16 [8192, 1536], P(('dp', 'ep'))
- expert_ids: int32 [8192, 6], P(('dp', 'ep'))
- gate_vals: float32 [8192, 6], P(('dp', 'ep'))
- slots: int32 [8192, 6], P(('dp', 'ep'))
- shared_w1: bfloat16 [1536, 1024], replicated
- shared_w3: bfloat16 [1536, 1024], replicated
- shared_w2: bfloat16 [1024, 1536], replicated
- shared_gate: bfloat16 [1536], replicated
- expert_w1: bfloat16 [64, 1536, 512], P('ep')
- expert_w3: bfloat16 [64, 1536, 512], P('ep')
- expert_w2: bfloat16 [64, 512, 1536], P('ep')
Outputs:
- output: bfloat16 [8192, 1536], P(('dp', 'ep'))
All inputs are finite; a program needn't handle non-finite values.
Results may differ from the reference program's by a relative error of at most 0.00516558.
Values are sent between devices in bfloat16 or wider.
A program may use at most 768 MiB of HBM per device.

```python
import jax
import jax.numpy as jnp
from jax import lax

EP_SIZE = 32
TOKENS_DEV = 256
HIDDEN = 1536
EXPERTS = 64
TOP_K = 6
EXPERT_FF = 512
SHARED_FF = 1024
CAPACITY = 48

NUM_TOKENS = EP_SIZE * TOKENS_DEV
BUF_ROWS = EXPERTS * CAPACITY


def draw_routes(route_key):
    score_key, bias_key, hot_key = jax.random.split(route_key, 3)
    scores = jax.random.randint(score_key, (NUM_TOKENS, EXPERTS), 0, 4096)
    expert_bias = jax.random.randint(bias_key, (EXPERTS,), 0, 1024)
    hot_expert = jax.random.randint(hot_key, (), 0, EXPERTS)
    expert_pos = jnp.arange(EXPERTS)
    forced = ((jnp.arange(NUM_TOKENS) % 2) == 0)[:, None] & (expert_pos[None, :] == hot_expert)
    total_score = scores + expert_bias[None, :] + jnp.where(forced, 8192, 0)
    distinct = total_score * EXPERTS + expert_pos[None, :]
    return lax.top_k(distinct, TOP_K)[1].astype(jnp.int32)


def source_slots(src_ids):
    flat_ids = src_ids.reshape(TOKENS_DEV * TOP_K)
    one_hot = (flat_ids[:, None] == jnp.arange(EXPERTS)[None, :]).astype(jnp.int32)
    earlier = jnp.cumsum(one_hot, axis=0) - one_hot
    position = jnp.sum(earlier * one_hot, axis=1)
    return jnp.where(position < CAPACITY, position, -1).reshape(TOKENS_DEV, TOP_K).astype(jnp.int32)


def normal_stack(stack_key, rows, cols):
    def one_matrix(one_key):
        return (jax.random.normal(one_key, (rows, cols), jnp.float32) * rows ** -0.5).astype(jnp.bfloat16)
    return lax.map(one_matrix, jax.random.split(stack_key, EXPERTS))


def setup_inputs(seed: int = 0, part: int = 0) -> dict:
    part_key = jax.random.fold_in(jax.random.key(seed), part)
    tok_key, route_key, gate_key = jax.random.split(part_key, 3)
    weight_keys = jax.random.split(jax.random.key(seed + 1), 7)
    tokens = jax.random.normal(tok_key, (NUM_TOKENS, HIDDEN), jnp.float32).astype(jnp.bfloat16)
    expert_ids = draw_routes(route_key)
    slots = lax.map(source_slots, expert_ids.reshape(EP_SIZE, TOKENS_DEV, TOP_K)).reshape(NUM_TOKENS, TOP_K)
    gate_vals = jax.random.uniform(gate_key, (NUM_TOKENS, TOP_K), jnp.float32, 0.5, 1.5) * TOP_K ** -0.5
    shared_w1 = (jax.random.normal(weight_keys[0], (HIDDEN, SHARED_FF), jnp.float32) * HIDDEN ** -0.5).astype(jnp.bfloat16)
    shared_w3 = (jax.random.normal(weight_keys[1], (HIDDEN, SHARED_FF), jnp.float32) * HIDDEN ** -0.5).astype(jnp.bfloat16)
    shared_w2 = (jax.random.normal(weight_keys[2], (SHARED_FF, HIDDEN), jnp.float32) * SHARED_FF ** -0.5).astype(jnp.bfloat16)
    shared_gate = (jax.random.normal(weight_keys[3], (HIDDEN,), jnp.float32) * 2.0 * HIDDEN ** -0.5).astype(jnp.bfloat16)
    expert_w1 = normal_stack(weight_keys[4], HIDDEN, EXPERT_FF)
    expert_w3 = normal_stack(weight_keys[5], HIDDEN, EXPERT_FF)
    expert_w2 = normal_stack(weight_keys[6], EXPERT_FF, HIDDEN)
    return {'tokens': tokens, 'expert_ids': expert_ids, 'gate_vals': gate_vals, 'slots': slots, 'shared_w1': shared_w1, 'shared_w3': shared_w3, 'shared_w2': shared_w2, 'shared_gate': shared_gate, 'expert_w1': expert_w1, 'expert_w3': expert_w3, 'expert_w2': expert_w2}


def swiglu_rows(rows, w_up, w_in, w_down):
    act_a = jnp.dot(rows, w_up, preferred_element_type=jnp.float32)
    act_b = jnp.dot(rows, w_in, preferred_element_type=jnp.float32)
    hidden_act = (jax.nn.silu(act_a) * act_b).astype(jnp.bfloat16)
    return jnp.dot(hidden_act, w_down, preferred_element_type=jnp.float32)


def reference(tokens, expert_ids, gate_vals, slots, shared_w1, shared_w3, shared_w2, shared_gate, expert_w1, expert_w3, expert_w2):
    src_tokens = tokens.reshape(EP_SIZE, TOKENS_DEV, HIDDEN)
    kept_mask = slots >= 0
    slot_dest = jnp.where(kept_mask, expert_ids * CAPACITY + slots, BUF_ROWS)
    flat_dest = slot_dest.reshape(EP_SIZE, TOKENS_DEV * TOP_K)
    copy_tok = jnp.arange(TOKENS_DEV * TOP_K, dtype=jnp.int32) // TOP_K

    def dispatch_one(operands):
        src_rows, src_dest = operands
        row_owner = jnp.full((BUF_ROWS + 1,), TOKENS_DEV, jnp.int32).at[src_dest].set(copy_tok)
        return jnp.take(src_rows, row_owner[:BUF_ROWS], axis=0, mode='fill', fill_value=0)

    buffers = lax.map(dispatch_one, (src_tokens, flat_dest))
    per_expert = buffers.reshape(EP_SIZE, EXPERTS, CAPACITY, HIDDEN).transpose(1, 0, 2, 3).reshape(EXPERTS, EP_SIZE * CAPACITY, HIDDEN)

    def expert_one(operands):
        rows, w_up, w_in, w_down = operands
        return swiglu_rows(rows, w_up, w_in, w_down).astype(jnp.bfloat16)

    expert_out = lax.map(expert_one, (per_expert, expert_w1, expert_w3, expert_w2))
    returned = expert_out.reshape(EXPERTS, EP_SIZE, CAPACITY, HIDDEN).transpose(1, 0, 2, 3).reshape(EP_SIZE, BUF_ROWS, HIDDEN)
    weights = jnp.where(kept_mask, gate_vals, 0.0).reshape(EP_SIZE, TOKENS_DEV, TOP_K)
    src_dest = slot_dest.reshape(EP_SIZE, TOKENS_DEV, TOP_K)

    def combine_one(operands):
        src_rows, src_out, src_idx, src_weights = operands
        picked = jnp.take(src_out, src_idx, axis=0, mode='fill', fill_value=0)
        routed = jnp.einsum('tk,tkd->td', src_weights, picked.astype(jnp.float32))
        gate_logit = jnp.dot(src_rows, shared_gate, preferred_element_type=jnp.float32)
        shared_out = jax.nn.sigmoid(gate_logit)[:, None] * swiglu_rows(src_rows, shared_w1, shared_w3, shared_w2)
        return (src_rows.astype(jnp.float32) + shared_out + routed).astype(jnp.bfloat16)

    result = lax.map(combine_one, (src_tokens, returned, src_dest, weights))
    return result.reshape(NUM_TOKENS, HIDDEN)
```

```python
import functools
import math

import jax
import jax.numpy as jnp
from jax import lax
from jax.experimental import pallas as pl
from jax.experimental.pallas import tpu as pltpu
from jax.sharding import PartitionSpec as P

MESH = pl.DeviceIdType.MESH
VMEM_LIMIT = 67043328
F32, BF16 = jnp.float32, jnp.bfloat16

DIRS = ((0, 1), (0, -1), (1, 1), (1, -1))


def wrap(v):
    return (v + 1) % 4 - 1


def shift(axis, way, at):
    moved = list(at)
    moved[axis] = wrap(moved[axis] - way)
    return tuple(moved)


def ahead_piece(way):
    return 0 if way > 0 else 1


def plan_gather():
    queues = [[] for _ in DIRS]
    first = []
    for d, (axis, way) in enumerate(DIRS):
        for half in (axis, 1 - axis):
            for p in (ahead_piece(way), 1 - ahead_piece(way)):
                queues[d].append((half, (0, 0), p))
                first.append((d, (half, (0, 0), p)))
    steps = []
    while any(queues):
        moved = [q.pop(0) if q else None for q in queues]
        arrivals = []
        for d, piece in enumerate(moved):
            if piece is None:
                continue
            half, at, p = piece
            axis, way = DIRS[d]
            at = shift(axis, way, at)
            onward = []
            if p == ahead_piece(way) and abs(at[axis]) == 1:
                onward.append(d)
            if axis == half:
                onward += [e for e, (other, _) in enumerate(DIRS) if other != axis]
            for e in onward:
                queues[e].append((half, at, p))
            arrivals.append((d, (half, at, p), onward))
        steps.append(arrivals)
    return first, steps


def plan_units(steps, chips_per_unit=2):
    done = {(0, 0): 0}
    for i, arrivals in enumerate(steps):
        for _, (_, at, _), _ in arrivals:
            done[at] = i + 1
    order = sorted(done, key=lambda at: (done[at], at))
    units = [order[i : i + chips_per_unit] for i in range(0, len(order), chips_per_unit)]
    return units, [max(done[at] for at in unit) for unit in units]


def carries_meta(piece):
    half, _, p = piece
    return half == 0 and p == 0


def place(side):
    me = lax.axis_index('ep')
    chip = me // 2
    return me, lax.rem(chip, side), chip // side, lax.rem(me, 2)


def pick(table, i):
    out = i * 0 + table[0]
    for k in range(1, len(table)):
        out = jnp.where(i == k, table[k], out)
    return out


def silu_gate(a, b):
    return (jax.nn.silu(a) * b).astype(BF16)


def gather_kernel(side, capacity, top_k, tok_in, meta_in, sw1_in, sw3_in, sw2_in, sg_ref, w1_in, w3_in, w2_in,
                  r_out, meta, base,
                  tok, w1, w3, w2, sw1, sw3, sw2, xe, rows_out,
                  load_sem, link_send, chip_send, recv, meta_link_send, meta_chip_send, meta_recv, out_sem):
    me, x, y, c = place(side)
    first, steps = plan_gather()
    units, ready = plan_units(steps)
    link_order = [[piece for e, piece in first if e == d] for d in range(4)]
    chip_order = [(half, (0, 0), p) for half in range(2) for p in range(2)]
    for arrivals in steps:
        for _, piece, onward in arrivals:
            chip_order.append(piece)
            for e in onward:
                link_order[e].append(piece)
    meta_order = [[piece for piece in link_order[d] if carries_meta(piece)] for d in range(4)]
    meta_chip_order = [piece for piece in chip_order if carries_meta(piece)]
    n_tok, hidden = tok_in.shape
    half_cols, half_rows = hidden // 2, n_tok // 2
    pair = 2 * capacity

    def device(at, core=None):
        dx, dy = at
        col, row = lax.rem(x + (dx + side), side), lax.rem(y + (dy + side), side)
        return (row * side + col) * 2 + (c if core is None else core)

    def neighbour(d):
        axis, way = DIRS[d]
        return device((way, 0) if axis == 0 else (0, way))

    partner = me + 1 - 2 * c

    loads = [pltpu.make_async_copy(tok_in, tok.at[me], load_sem.at[0]),
             pltpu.make_async_copy(meta_in, meta.at[me], load_sem.at[1]),
             pltpu.make_async_copy(sw1_in, sw1, load_sem.at[2]),
             pltpu.make_async_copy(sw3_in, sw3, load_sem.at[3]),
             pltpu.make_async_copy(sw2_in, sw2, load_sem.at[4]),
             pltpu.make_async_copy(w1_in, w1, load_sem.at[5]),
             pltpu.make_async_copy(w3_in, w3, load_sem.at[6]),
             pltpu.make_async_copy(w2_in, w2, load_sem.at[7])]
    for load in loads:
        load.start()

    barrier = pltpu.get_barrier_semaphore()
    for to in [neighbour(d) for d in range(4)] + [partner]:
        pl.semaphore_signal(barrier, inc=1, device_id={'ep': to}, device_id_type=MESH)
    pl.semaphore_wait(barrier, 5)
    loads[0].wait()
    loads[1].wait()

    def view(half, src, p):
        return tok.at[src, pl.ds(p * half_rows, half_rows), pl.ds(half * half_cols, half_cols)]

    def rdma(src, dst, send, arrive, to):
        return pltpu.make_async_remote_copy(src_ref=src, dst_ref=dst, send_sem=send, recv_sem=arrive,
                                            device_id={'ep': to}, device_id_type=MESH)

    def piece_copy(piece, src, send, to):
        half, _, p = piece
        return rdma(view(half, src, p), view(half, src, p), send, recv.at[src, half * 2 + p], to)

    def meta_copy(src, send, to):
        return rdma(meta.at[src], meta.at[src], send, meta_recv.at[src], to)

    def send_link(d, piece):
        src = device(piece[1])
        piece_copy(piece, src, link_send.at[d, link_order[d].index(piece)], neighbour(d)).start()
        if carries_meta(piece):
            meta_copy(src, meta_link_send.at[d, meta_order[d].index(piece)], neighbour(d)).start()

    def send_chip(piece):
        src = device(piece[1])
        piece_copy(piece, src, chip_send.at[chip_order.index(piece)], partner).start()
        if carries_meta(piece):
            meta_copy(src, meta_chip_send.at[meta_chip_order.index(piece)], partner).start()

    def await_piece(piece, core):
        src = device(piece[1], core)
        piece_copy(piece, src, link_send.at[0, 0], partner).wait_recv()
        if carries_meta(piece):
            meta_copy(src, meta_link_send.at[0, 0], partner).wait_recv()

    def do_step(i):
        for d, piece, onward in steps[i]:
            await_piece(piece, None)
            for e in onward:
                send_link(e, piece)
            send_chip(piece)

    for d, piece in first:
        send_link(d, piece)
    for half in range(2):
        for p in range(2):
            send_chip((half, (0, 0), p))

    for load in loads[2:5]:
        load.wait()
    x_own = tok[me]
    tile = 256
    base[...] = jnp.zeros_like(base)

    def shared_tile(n, _):
        cols = pl.ds(pl.multiple_of(n * tile, tile), tile)
        a = jnp.dot(x_own, sw1[:, cols], preferred_element_type=F32)
        b = jnp.dot(x_own, sw3[:, cols], preferred_element_type=F32)
        base[...] += jnp.dot(silu_gate(a, b), sw2[cols, :], preferred_element_type=F32)
        return 0

    lax.fori_loop(0, sw1.shape[1] // tile, shared_tile, 0)
    x_f32 = x_own.astype(F32)
    logit = jnp.sum(x_f32 * sg_ref[...].astype(F32), axis=1, keepdims=True)
    base[...] = x_f32 + jax.nn.sigmoid(logit) * base[...]
    for load in loads[5:]:
        load.wait()

    row_ids = lax.broadcasted_iota(jnp.int32, (pair, n_tok), 0)
    target = (row_ids + me * pair).astype(F32)
    n_src = 4

    def unit_device(u, i):
        dx = pick([unit[i // 2][0] + side for unit in units], u)
        dy = pick([unit[i // 2][1] + side for unit in units], u)
        col, row = lax.rem(x + dx, side), lax.rem(y + dy, side)
        return (row * side + col) * 2 + i % 2

    def out_copies(slot, srcs):
        return [pltpu.make_async_copy(
                    rows_out.at[slot, j, pl.ds(i * capacity, capacity), pl.ds(h * half_cols, half_cols)],
                    r_out.at[h, srcs[i], pl.ds(j * capacity, capacity)],
                    out_sem.at[slot, (i * 2 + j) * 2 + h])
                for i in range(n_src) for j in range(2) for h in range(2)]

    def do_unit(u, _):
        done = 0
        for k, after in enumerate(ready):
            lo, hi = done, after
            done = after

            @pl.when(u == k)
            def _(lo=lo, hi=hi, k=k):
                for i in range(lo, hi):
                    do_step(i)
                for at in units[k]:
                    for half in range(2):
                        for p in range(2):
                            await_piece((half, at, p), 1 - c)

        slot = lax.rem(u, 2)
        srcs = [unit_device(u, i) for i in range(n_src)]

        @pl.when(u >= 2)
        def _():
            for copy in out_copies(slot, srcs):
                copy.wait()

        for i in range(n_src):
            codes = meta[srcs[i], 0:8, :]
            hit = codes[0:1, :] == target
            for k in range(1, top_k):
                hit = jnp.logical_or(hit, codes[k : k + 1, :] == target)
            one_hot = jnp.where(hit, 1.0, 0.0).astype(BF16)
            picked = jnp.dot(one_hot, tok[srcs[i]], preferred_element_type=F32).astype(BF16)
            xe[0, i * capacity : (i + 1) * capacity, :] = picked[:capacity]
            xe[1, i * capacity : (i + 1) * capacity, :] = picked[capacity:]

        def do_expert(j, _):
            a = jnp.dot(xe[j], w1[j], preferred_element_type=F32)
            b = jnp.dot(xe[j], w3[j], preferred_element_type=F32)
            rows_out[slot, j] = jnp.dot(silu_gate(a, b), w2[j], preferred_element_type=F32).astype(BF16)
            return 0

        lax.fori_loop(0, 2, do_expert, 0)
        for copy in out_copies(slot, srcs):
            copy.start()
        return 0

    n_units = len(units)
    lax.fori_loop(0, n_units, do_unit, 0)
    for u in range(n_units - 2, n_units):
        for copy in out_copies(u % 2, [me] * n_src):
            copy.wait()
    for d in range(4):
        for i, piece in enumerate(link_order[d]):
            piece_copy(piece, me, link_send.at[d, i], partner).wait_send()
        for i in range(len(meta_order[d])):
            meta_copy(me, meta_link_send.at[d, i], partner).wait_send()
    for i, piece in enumerate(chip_order):
        piece_copy(piece, me, chip_send.at[i], partner).wait_send()
    for i in range(len(meta_chip_order)):
        meta_copy(me, meta_chip_send.at[i], partner).wait_send()


def return_kernel(side, capacity, top_k, r_in, meta, base, y_out,
                  rows, relay, wt, part, hop1, hop2,
                  direct_send, relay_send, fwd_send, chip_send, local_sem, rows_recv, relay_recv,
                  hop1_send, hop1_recv, hop2_send, hop2_recv):
    me, x, y, c = place(side)
    n_tok = base.shape[0]
    half_cols, half_rows = base.shape[1] // 2, n_tok // 2
    pair = 2 * capacity
    order = (2, 1, -1, 0)

    def device(dx, dy, core):
        col, row = lax.rem(x + (dx + side), side), lax.rem(y + (dy + side), side)
        return (row * side + col) * 2 + core

    def along(h, a, b, core):
        return device(a, b, core) if h == 0 else device(b, a, core)

    partner = me + 1 - 2 * c
    here = (x, y)

    barrier = pltpu.get_barrier_semaphore()
    peers = [along(h, w, 0, core) for h in range(2) for w in (1, -1) for core in range(2)] + [partner]
    for to in peers:
        pl.semaphore_signal(barrier, inc=1, device_id={'ep': to}, device_id_type=MESH)
    pl.semaphore_wait(barrier, len(peers))

    def rdma(src, dst, send, arrive, to):
        return pltpu.make_async_remote_copy(src_ref=src, dst_ref=dst, send_sem=send, recv_sem=arrive,
                                            device_id={'ep': to}, device_id_type=MESH)

    def go(copy):
        copy.start()

    def entry(h, hops, core):
        return lax.rem(here[h] + (hops + side), side) * 2 + core

    def send_chunk(q):
        for h in range(2):
            b = order[q]
            for w, way in enumerate((1, -1)):
                go(rdma(r_in.at[h, along(h, 2, b, w)], relay.at[h, q, w], relay_send.at[h, q, w], relay_recv.at[h, q, w],
                        along(h, way, 0, c)))
        for h in range(2):
            b = order[q]
            mine = entry(h, 0, c)
            for w, way in enumerate((1, -1)):
                for core in range(2):
                    go(rdma(r_in.at[h, along(h, way, b, core)], rows.at[h, q, mine], direct_send.at[h, q, w * 2 + core],
                            rows_recv.at[h, q, mine], along(h, way, 0, core)))
            go(rdma(r_in.at[h, along(h, 0, b, 1 - c)], rows.at[h, q, mine], chip_send.at[h, q], rows_recv.at[h, q, mine],
                    partner))
            own = pltpu.make_async_copy(r_in.at[h, along(h, 0, b, c)], rows.at[h, q, mine], local_sem.at[h, q])
            own.start()

    def forward(q):
        for h in range(2):
            for w, way in enumerate((1, -1)):
                rdma(relay.at[h, q, w], relay.at[h, q, w], relay_send.at[h, q, w], relay_recv.at[h, q, w],
                     partner).wait_recv()
                src = entry(h, -way, c)
                go(rdma(relay.at[h, q, w], rows.at[h, q, src], fwd_send.at[h, q, w], rows_recv.at[h, q, src],
                        along(h, way, 0, w)))

    def await_rows(h, q):
        mine = entry(h, 0, c)
        pltpu.make_async_copy(r_in.at[h, me], rows.at[h, q, mine], local_sem.at[h, q]).wait()
        for hops in (0, 1, -1, 2):
            for core in range(2):
                if hops == 0:
                    if core == 1:
                        continue
                    src = entry(h, 0, 1 - c)
                else:
                    src = entry(h, hops, core)
                rdma(r_in.at[h, me], rows.at[h, q, src], chip_send.at[h, q], rows_recv.at[h, q, src], partner).wait_recv()

    def second(h, way):
        return along(h, 0, way, c)

    def hop1_copy(h, w):
        way = (1, -1)[w]
        return rdma(part.at[h, 0, pl.ds(w * half_rows, half_rows)], hop1.at[h, w], hop1_send.at[h, w], hop1_recv.at[h, w],
                    second(h, way))

    def hop2_copy(h, w, p):
        way = (1, -1)[w]
        piece = pl.ds(p * half_rows, half_rows)
        return rdma(part.at[h, 1 + w, piece], hop2.at[h, w, piece], hop2_send.at[h, w, p], hop2_recv.at[h, w, p],
                    second(h, way))

    send_chunk(0)
    send_chunk(1)

    row_ids = lax.broadcasted_iota(jnp.int32, (pair, n_tok), 0)

    def combine(n, _):
        q, h = n // 2, lax.rem(n, 2)
        for k in range(4):
            @pl.when(n == 2 * k)
            def _(k=k):
                forward(k)
                if k + 2 < 4:
                    send_chunk(k + 2)
            for hh in range(2):
                @pl.when(n == 2 * k + hh)
                def _(k=k, hh=hh):
                    await_rows(hh, k)
        b = pick([o + side for o in order], q)
        bx, by = lax.rem(x + jnp.where(h == 0, 0, b), side), lax.rem(y + jnp.where(h == 0, b, 0), side)
        dest = (by * side + bx) * 2 + c
        codes = meta[dest, 0:8, :]
        gates = meta[dest, 8:16, :]

        def weights(g, _):
            gx, gy = jnp.where(h == 0, g // 2, x), jnp.where(h == 0, y, g // 2)
            source = (gy * side + gx) * 2 + lax.rem(g, 2)
            target = (row_ids + source * pair).astype(F32)
            w = jnp.where(codes[0:1, :] == target, gates[0:1, :], 0.0)
            for k in range(1, top_k):
                w = jnp.where(codes[k : k + 1, :] == target, gates[k : k + 1, :], w)
            at = pl.ds(pl.multiple_of(g * pair, pair), pair)
            hi = w.astype(BF16)
            w = w - hi.astype(F32)
            mid = w.astype(BF16)
            wt[0, at, :] = hi
            wt[1, at, :] = mid
            wt[2, at, :] = (w - mid.astype(F32)).astype(BF16)
            return 0

        lax.fori_loop(0, 2 * side, weights, 0)
        block = rows[h, q].reshape(2 * side * pair, half_cols)
        dims = (((0,), (0,)), ((), ()))
        total = lax.dot_general(wt[2], block, dims, preferred_element_type=F32)
        total += lax.dot_general(wt[1], block, dims, preferred_element_type=F32)
        total += lax.dot_general(wt[0], block, dims, preferred_element_type=F32)
        part[h, q] = total

        for hh in range(2):
            @pl.when(n == hh)
            def _(hh=hh):
                for w in range(2):
                    hop1_copy(hh, w).start()
            for w in range(2):
                @pl.when(n == 2 * (1 + w) + hh)
                def _(hh=hh, w=w):
                    hop2_copy(hh, w, 1 - w).start()
                    hop1_copy(hh, w).wait_recv()
                    own = pl.ds(w * half_rows, half_rows)
                    part[hh, 1 + w, own] += hop1[hh, w]
                    hop2_copy(hh, w, w).start()
        return 0

    lax.fori_loop(0, 8, combine, 0)
    for h in range(2):
        for w in range(2):
            for p in range(2):
                hop2_copy(h, w, p).wait_recv()
        cols = slice(h * half_cols, (h + 1) * half_cols)
        y_out[:, cols] = (base[:, cols] + (part[h, 3] + (hop2[h, 0] + hop2[h, 1]))).astype(BF16)
    for h in range(2):
        for q in range(4):
            sems = [relay_send.at[h, q, w] for w in range(2)] + [fwd_send.at[h, q, w] for w in range(2)]
            sems += [direct_send.at[h, q, k] for k in range(4)] + [chip_send.at[h, q]]
            for sem in sems:
                rdma(r_in.at[h, me], rows.at[h, q, 0], sem, rows_recv.at[h, q, 0], partner).wait_send()
        for w in range(2):
            hop1_copy(h, w).wait_send()
            for p in range(2):
                hop2_copy(h, w, p).wait_send()


def solution(mesh):
    num_ep = mesh.shape['ep']
    side = math.isqrt(num_ep // 2)
    assert side == 4 and 2 * side * side == num_ep
    row_spec = P(('dp', 'ep'), None)
    replicated = P()
    expert_spec = P('ep', None, None)
    vmem, anywhere = pl.BlockSpec(memory_space=pltpu.VMEM), pl.BlockSpec(memory_space=pl.ANY)
    dma = pltpu.SemaphoreType.DMA

    def device_step(tokens, expert_ids, gate_vals, slots, shared_w1, shared_w3, shared_w2, shared_gate, expert_w1, expert_w3, expert_w2):
        tok_count, hidden = tokens.shape
        top_k = expert_ids.shape[1]
        local_experts, _, ff = expert_w1.shape
        num_experts = local_experts * num_ep
        capacity = 8 * ((2 * tok_count * top_k + 8 * num_experts - 1) // (8 * num_experts))
        assert local_experts == 2 and top_k <= 8 and capacity % 16 == 0
        pair = local_experts * capacity
        half = hidden // 2
        code = jnp.where(slots >= 0, expert_ids * capacity + slots, -1).astype(F32)
        pad = ((0, 0), (0, 8 - top_k))
        meta = jnp.concatenate([jnp.pad(code, pad, constant_values=-1.0), jnp.pad(gate_vals, pad)], axis=1).T
        r, meta_all, base = pl.pallas_call(
            functools.partial(gather_kernel, side, capacity, top_k),
            out_shape=(jax.ShapeDtypeStruct((2, num_ep, pair, half), BF16),
                       jax.ShapeDtypeStruct((num_ep, 16, tok_count), F32),
                       jax.ShapeDtypeStruct((tok_count, hidden), F32)),
            in_specs=[anywhere] * 5 + [vmem] + [anywhere] * 3,
            out_specs=(anywhere, vmem, vmem),
            scratch_shapes=[
                pltpu.VMEM((num_ep, tok_count, hidden), BF16),
                pltpu.VMEM((local_experts, hidden, ff), BF16),
                pltpu.VMEM((local_experts, hidden, ff), BF16),
                pltpu.VMEM((local_experts, ff, hidden), BF16),
                pltpu.VMEM(shared_w1.shape, BF16),
                pltpu.VMEM(shared_w3.shape, BF16),
                pltpu.VMEM(shared_w2.shape, BF16),
                pltpu.VMEM((local_experts, 4 * capacity, hidden), BF16),
                pltpu.VMEM((2, local_experts, 4 * capacity, hidden), BF16),
                dma((8,)), dma((4, 15)), dma((64,)), dma((num_ep, 4)), dma((4, 15)), dma((16,)), dma((num_ep,)),
                dma((2, 16)),
            ],
            compiler_params=pltpu.CompilerParams(collective_id=0, has_side_effects=True, vmem_limit_bytes=VMEM_LIMIT),
            name='gather_experts',
        )(tokens, meta, shared_w1, shared_w3, shared_w2, shared_gate.reshape(1, hidden), expert_w1, expert_w3, expert_w2)
        return pl.pallas_call(
            functools.partial(return_kernel, side, capacity, top_k),
            out_shape=jax.ShapeDtypeStruct((tok_count, hidden), BF16),
            in_specs=[anywhere, vmem, vmem],
            out_specs=vmem,
            scratch_shapes=[
                pltpu.VMEM((2, 4, 2 * side, pair, half), BF16),
                pltpu.VMEM((2, 4, 2, pair, half), BF16),
                pltpu.VMEM((3, 2 * side * pair, tok_count), BF16),
                pltpu.VMEM((2, 4, tok_count, half), F32),
                pltpu.VMEM((2, 2, tok_count // 2, half), F32),
                pltpu.VMEM((2, 2, tok_count, half), F32),
                dma((2, 4, 4)), dma((2, 4, 2)), dma((2, 4, 2)), dma((2, 4)), dma((2, 4)), dma((2, 4, 2 * side)),
                dma((2, 4, 2)), dma((2, 2)), dma((2, 2)), dma((2, 2, 2)), dma((2, 2, 2)),
            ],
            compiler_params=pltpu.CompilerParams(collective_id=1, has_side_effects=True, vmem_limit_bytes=VMEM_LIMIT),
            name='return_combine',
        )(r, meta_all, base)

    return jax.shard_map(device_step, mesh=mesh, in_specs=(row_spec, row_spec, row_spec, row_spec, replicated, replicated, replicated, replicated, expert_spec, expert_spec, expert_spec), out_specs=row_spec, check_vma=False)
```

```python
import functools
import math

import jax
import jax.numpy as jnp
from jax import lax
from jax.experimental import pallas as pl
from jax.experimental.pallas import tpu as pltpu
from jax.sharding import PartitionSpec as P

MESH = pl.DeviceIdType.MESH
VMEM_LIMIT = 67043328
F32, BF16 = jnp.float32, jnp.bfloat16

DIRS = ((0, 1), (0, -1), (1, 1), (1, -1))


def wrap(v):
    return (v + 1) % 4 - 1


def shift(axis, way, at):
    moved = list(at)
    moved[axis] = wrap(moved[axis] - way)
    return tuple(moved)


def ahead_piece(way):
    return 0 if way > 0 else 1


def plan_gather():
    queues = [[] for _ in DIRS]
    first = []
    for d, (axis, way) in enumerate(DIRS):
        for half in (axis, 1 - axis):
            for p in (ahead_piece(way), 1 - ahead_piece(way)):
                queues[d].append((half, (0, 0), p))
                first.append((d, (half, (0, 0), p)))
    steps = []
    while any(queues):
        moved = [q.pop(0) if q else None for q in queues]
        arrivals = []
        for d, piece in enumerate(moved):
            if piece is None:
                continue
            half, at, p = piece
            axis, way = DIRS[d]
            at = shift(axis, way, at)
            onward = []
            if p == ahead_piece(way) and abs(at[axis]) == 1:
                onward.append(d)
            if axis == half:
                onward += [e for e, (other, _) in enumerate(DIRS) if other != axis]
            for e in onward:
                queues[e].append((half, at, p))
            arrivals.append((d, (half, at, p), onward))
        steps.append(arrivals)
    return first, steps


def plan_units(steps, chips_per_unit=2):
    done = {(0, 0): 0}
    for i, arrivals in enumerate(steps):
        for _, (_, at, _), _ in arrivals:
            done[at] = i + 1
    order = sorted(done, key=lambda at: (done[at], at))
    units = [order[i : i + chips_per_unit] for i in range(0, len(order), chips_per_unit)]
    return units, [max(done[at] for at in unit) for unit in units]


def carries_meta(piece):
    half, _, p = piece
    return half == 0 and p == 0


def place(side):
    me = lax.axis_index('ep')
    chip = me // 2
    return me, lax.rem(chip, side), chip // side, lax.rem(me, 2)


def pick(table, i):
    out = i * 0 + table[0]
    for k in range(1, len(table)):
        out = jnp.where(i == k, table[k], out)
    return out


def silu_gate(a, b):
    return (jax.nn.silu(a) * b).astype(BF16)


def layer_kernel(side, capacity, tok_in, ids_ref, slots_ref, gates_ref, sw1_in, sw3_in, sw2_in, sg_ref, w1_in, w3_in, w2_in,
                 y_out, r_buf, relay,
                 tok, meta, base, w1, w3, w2, xe, rows, wt, part, hop1, hop2,
                 load_sem, link_send, chip_send, recv, meta_link_send, meta_chip_send, meta_recv, out_sem,
                 direct_send, relay_send, fwd_send, pair_send, local_sem, rows_recv, relay_recv,
                 hop1_send, hop1_recv, hop2_send, hop2_recv):
    me, x, y, c = place(side)
    first, steps = plan_gather()
    units, ready = plan_units(steps)
    link_order = [[piece for e, piece in first if e == d] for d in range(4)]
    chip_order = [(half, (0, 0), p) for half in range(2) for p in range(2)]
    for arrivals in steps:
        for _, piece, onward in arrivals:
            chip_order.append(piece)
            for e in onward:
                link_order[e].append(piece)
    meta_order = [[piece for piece in link_order[d] if carries_meta(piece)] for d in range(4)]
    meta_chip_order = [piece for piece in chip_order if carries_meta(piece)]
    top_k = ids_ref.shape[0]
    n_tok, hidden = tok_in.shape
    half_cols, half_rows = hidden // 2, n_tok // 2
    ff = w1.shape[2]
    pair = 2 * capacity
    here = (x, y)

    def device(at, core=None):
        dx, dy = at
        col, row = lax.rem(x + (dx + side), side), lax.rem(y + (dy + side), side)
        return (row * side + col) * 2 + (c if core is None else core)

    def along(h, a, b, core):
        return device((a, b) if h == 0 else (b, a), core)

    def neighbour(d, core=None):
        axis, way = DIRS[d]
        return device((way, 0) if axis == 0 else (0, way), core)

    def rdma(src, dst, send, arrive, to):
        return pltpu.make_async_remote_copy(src_ref=src, dst_ref=dst, send_sem=send, recv_sem=arrive,
                                            device_id={'ep': to}, device_id_type=MESH)

    partner = me + 1 - 2 * c

    tok_load = pltpu.make_async_copy(tok_in, tok.at[me], load_sem.at[0])
    tok_load.start()
    shared_loads, expert_loads = [], []
    for j in range(2):
        cols = pl.ds(j * ff, ff)
        shared_loads += [pltpu.make_async_copy(sw1_in.at[:, cols], w1.at[j], load_sem.at[1 + j]),
                         pltpu.make_async_copy(sw3_in.at[:, cols], w3.at[j], load_sem.at[3 + j]),
                         pltpu.make_async_copy(sw2_in.at[cols], w2.at[j], load_sem.at[5 + j])]
    for k, (src, dst) in enumerate(((w1_in, w1), (w3_in, w3), (w2_in, w2))):
        expert_loads.append(pltpu.make_async_copy(src, dst, load_sem.at[7 + k]))
    for load in shared_loads:
        load.start()

    barrier = pltpu.get_barrier_semaphore()
    for to in [neighbour(d, core) for d in range(4) for core in range(2)] + [partner]:
        pl.semaphore_signal(barrier, inc=1, device_id={'ep': to}, device_id_type=MESH)
    slot_of = slots_ref[...]
    meta[me, 0:top_k, :] = jnp.where(slot_of >= 0, ids_ref[...] * capacity + slot_of, -1).astype(F32)
    meta[me, 8 : 8 + top_k, :] = gates_ref[...]
    meta[me, top_k:8, :] = jnp.full((8 - top_k, n_tok), -1.0, F32)
    meta[me, 8 + top_k : 16, :] = jnp.zeros((8 - top_k, n_tok), F32)
    tok_load.wait()
    pl.semaphore_wait(barrier, 9)

    def view(half, src, p):
        return tok.at[src, pl.ds(p * half_rows, half_rows), pl.ds(half * half_cols, half_cols)]

    def piece_copy(piece, src, send, to):
        half, _, p = piece
        return rdma(view(half, src, p), view(half, src, p), send, recv.at[src, half * 2 + p], to)

    def meta_copy(src, send, to):
        return rdma(meta.at[src], meta.at[src], send, meta_recv.at[src], to)

    def send_link(d, piece):
        src = device(piece[1])
        piece_copy(piece, src, link_send.at[d, link_order[d].index(piece)], neighbour(d)).start()
        if carries_meta(piece):
            meta_copy(src, meta_link_send.at[d, meta_order[d].index(piece)], neighbour(d)).start()

    def send_chip(piece):
        src = device(piece[1])
        piece_copy(piece, src, chip_send.at[chip_order.index(piece)], partner).start()
        if carries_meta(piece):
            meta_copy(src, meta_chip_send.at[meta_chip_order.index(piece)], partner).start()

    def await_piece(piece, core):
        src = device(piece[1], core)
        piece_copy(piece, src, link_send.at[0, 0], partner).wait_recv()
        if carries_meta(piece):
            meta_copy(src, meta_link_send.at[0, 0], partner).wait_recv()

    def do_step(i):
        for d, piece, onward in steps[i]:
            await_piece(piece, None)
            for e in onward:
                send_link(e, piece)
            send_chip(piece)

    order = (2, 1, -1, 0)

    def entry(h, hops, core):
        return lax.rem(here[h] + (hops + side), side) * 2 + core

    def send_relay(q):
        for h in range(2):
            for w, way in enumerate((1, -1)):
                rdma(r_buf.at[h, along(h, 2, order[q], w)], relay.at[h, q, w], relay_send.at[h, q, w],
                     relay_recv.at[h, q, w], along(h, way, 0, c)).start()

    def send_direct(q):
        b = order[q]
        for h in range(2):
            mine = entry(h, 0, c)
            for w, way in enumerate((1, -1)):
                for core in range(2):
                    rdma(r_buf.at[h, along(h, way, b, core)], rows.at[h, q, mine], direct_send.at[h, q, w * 2 + core],
                         rows_recv.at[h, q, mine], along(h, way, 0, core)).start()
            rdma(r_buf.at[h, along(h, 0, b, 1 - c)], rows.at[h, q, mine], pair_send.at[h, q], rows_recv.at[h, q, mine],
                 partner).start()
            pltpu.make_async_copy(r_buf.at[h, along(h, 0, b, c)], rows.at[h, q, mine], local_sem.at[h, q]).start()

    def forward(q):
        for h in range(2):
            for w, way in enumerate((1, -1)):
                rdma(relay.at[h, q, w], relay.at[h, q, w], relay_send.at[h, q, w], relay_recv.at[h, q, w],
                     partner).wait_recv()
                src = entry(h, -way, c)
                rdma(relay.at[h, q, w], rows.at[h, q, src], fwd_send.at[h, q, w], rows_recv.at[h, q, src],
                     along(h, way, 0, w)).start()

    def await_rows(h, q):
        pltpu.make_async_copy(r_buf.at[h, me], rows.at[h, q, entry(h, 0, c)], local_sem.at[h, q]).wait()
        sources = [entry(h, 0, 1 - c)] + [entry(h, hops, core) for hops in (1, -1, 2) for core in range(2)]
        for src in sources:
            rdma(r_buf.at[h, me], rows.at[h, q, src], pair_send.at[h, q], rows_recv.at[h, q, src], partner).wait_recv()

    def hop1_copy(h, w):
        return rdma(part.at[h, 0, pl.ds(w * half_rows, half_rows)], hop1.at[h, w], hop1_send.at[h, w], hop1_recv.at[h, w],
                    along(h, 0, (1, -1)[w], c))

    def hop2_copy(h, w, p):
        piece = pl.ds(p * half_rows, half_rows)
        return rdma(part.at[h, 1 + w, piece], hop2.at[h, w, piece], hop2_send.at[h, w, p], hop2_recv.at[h, w, p],
                    along(h, 0, (1, -1)[w], c))

    for d, piece in first:
        send_link(d, piece)
    for piece in chip_order[:4]:
        send_chip(piece)

    for load in shared_loads:
        load.wait()
    base[...] = jnp.zeros_like(base)

    def shared_piece(j, _):
        rows_in = tok[me]
        a = jnp.dot(rows_in, w1[j], preferred_element_type=F32)
        b = jnp.dot(rows_in, w3[j], preferred_element_type=F32)
        out = jnp.dot(silu_gate(a, b), w2[j], preferred_element_type=F32)
        for h in range(2):
            base[h] += out[:, h * half_cols : (h + 1) * half_cols]
        return 0

    lax.fori_loop(0, 2, shared_piece, 0)
    for load in expert_loads:
        load.start()
    x_f32 = tok[me].astype(F32)
    logit = jnp.sum(x_f32 * sg_ref[...].astype(F32), axis=1, keepdims=True)
    for h in range(2):
        base[h] = x_f32[:, h * half_cols : (h + 1) * half_cols] + jax.nn.sigmoid(logit) * base[h]
    for load in expert_loads:
        load.wait()

    row_ids = lax.broadcasted_iota(jnp.int32, (pair, n_tok), 0)
    target = (row_ids + me * pair).astype(F32)
    n_src = 4

    def unit_device(u, i):
        dx = pick([unit[i // 2][0] + side for unit in units], u)
        dy = pick([unit[i // 2][1] + side for unit in units], u)
        col, row = lax.rem(x + dx, side), lax.rem(y + dy, side)
        return (row * side + col) * 2 + i % 2

    def out_copies(slot, srcs):
        return [pltpu.make_async_copy(
                    xe.at[slot, j, pl.ds(i * capacity, capacity), pl.ds(h * half_cols, half_cols)],
                    r_buf.at[h, srcs[i], pl.ds(j * capacity, capacity)],
                    out_sem.at[slot, (i * 2 + j) * 2 + h])
                for i in range(n_src) for j in range(2) for h in range(2)]

    n_units = len(units)

    def do_unit(u, _):
        done = 0
        for k, after in enumerate(ready):
            lo, hi = done, after
            done = after

            @pl.when(u == k)
            def _(lo=lo, hi=hi, k=k):
                for i in range(lo, hi):
                    do_step(i)
                for at in units[k]:
                    for half in range(2):
                        for p in range(2):
                            await_piece((half, at, p), 1 - c)

        slot = lax.rem(u, 2)
        srcs = [unit_device(u, i) for i in range(n_src)]
        for i in range(n_src):
            codes = meta[srcs[i], 0:8, :]
            hit = codes[0:1, :] == target
            for k in range(1, top_k):
                hit = jnp.logical_or(hit, codes[k : k + 1, :] == target)
            one_hot = jnp.where(hit, 1.0, 0.0).astype(BF16)
            picked = jnp.dot(one_hot, tok[srcs[i]], preferred_element_type=F32).astype(BF16)
            xe[slot, 0, i * capacity : (i + 1) * capacity, :] = picked[:capacity]
            xe[slot, 1, i * capacity : (i + 1) * capacity, :] = picked[capacity:]

        @pl.when(u >= 1)
        def _():
            for copy in out_copies(1 - slot, srcs):
                copy.wait()

        @pl.when(u == n_units - 3)
        def _():
            send_direct(1)
            send_direct(2)

        def do_expert(j, _):
            a = jnp.dot(xe[slot, j], w1[j], preferred_element_type=F32)
            b = jnp.dot(xe[slot, j], w3[j], preferred_element_type=F32)
            xe[slot, j] = jnp.dot(silu_gate(a, b), w2[j], preferred_element_type=F32).astype(BF16)
            return 0

        lax.fori_loop(0, 2, do_expert, 0)
        for copy in out_copies(slot, srcs):
            copy.start()
        return 0

    lax.fori_loop(0, n_units, do_unit, 0)
    for copy in out_copies((n_units - 1) % 2, [me] * n_src):
        copy.wait()
    send_relay(0)
    send_direct(0)
    send_relay(1)
    send_relay(2)

    def combine(n, _):
        q, h = n // 2, lax.rem(n, 2)

        @pl.when(n == 0)
        def _():
            forward(0)
            forward(1)
            forward(2)
            send_relay(3)

        @pl.when(n == 2)
        def _():
            send_direct(3)

        @pl.when(n == 6)
        def _():
            forward(3)
            for hh in range(2):
                for w in range(2):
                    hop1_copy(hh, w).wait_recv()
                    own = pl.ds(w * half_rows, half_rows)
                    part[hh, 1 + w, own] += hop1[hh, w]
                    hop2_copy(hh, w, w).start()

        for k in range(4):
            for hh in range(2):
                @pl.when(n == 2 * k + hh)
                def _(k=k, hh=hh):
                    await_rows(hh, k)
        b = pick([o + side for o in order], q)
        bx, by = lax.rem(x + jnp.where(h == 0, 0, b), side), lax.rem(y + jnp.where(h == 0, b, 0), side)
        dest = (by * side + bx) * 2 + c
        codes = meta[dest, 0:8, :]
        gates = meta[dest, 8:16, :]

        def weights(g, _):
            gx, gy = jnp.where(h == 0, g // 2, x), jnp.where(h == 0, y, g // 2)
            source = (gy * side + gx) * 2 + lax.rem(g, 2)
            goal = (row_ids + source * pair).astype(F32)
            w = jnp.where(codes[0:1, :] == goal, gates[0:1, :], 0.0)
            for k in range(1, top_k):
                w = jnp.where(codes[k : k + 1, :] == goal, gates[k : k + 1, :], w)
            at = pl.ds(pl.multiple_of(g * pair, pair), pair)
            hi = w.astype(BF16)
            w = w - hi.astype(F32)
            mid = w.astype(BF16)
            wt[0, at, :] = hi
            wt[1, at, :] = mid
            wt[2, at, :] = (w - mid.astype(F32)).astype(BF16)
            return 0

        lax.fori_loop(0, 2 * side, weights, 0)
        block = rows[h, q].reshape(2 * side * pair, half_cols)
        dims = (((0,), (0,)), ((), ()))
        total = lax.dot_general(wt[2], block, dims, preferred_element_type=F32)
        total += lax.dot_general(wt[1], block, dims, preferred_element_type=F32)
        total += lax.dot_general(wt[0], block, dims, preferred_element_type=F32)

        @pl.when(q < 3)
        def _():
            part[h, jnp.minimum(q, 2)] = total

        @pl.when(q == 3)
        def _():
            base[h] += total

        for hh in range(2):
            @pl.when(n == hh)
            def _(hh=hh):
                for w in range(2):
                    hop1_copy(hh, w).start()
            for w in range(2):
                @pl.when(n == 2 * (1 + w) + hh)
                def _(hh=hh, w=w):
                    hop2_copy(hh, w, 1 - w).start()
        return 0

    lax.fori_loop(0, 8, combine, 0)
    for h in range(2):
        for w in range(2):
            for p in range(2):
                hop2_copy(h, w, p).wait_recv()
        y_out[:, h * half_cols : (h + 1) * half_cols] = (base[h] + (hop2[h, 0] + hop2[h, 1])).astype(BF16)

    for d in range(4):
        for i, piece in enumerate(link_order[d]):
            piece_copy(piece, me, link_send.at[d, i], partner).wait_send()
        for i in range(len(meta_order[d])):
            meta_copy(me, meta_link_send.at[d, i], partner).wait_send()
    for i, piece in enumerate(chip_order):
        piece_copy(piece, me, chip_send.at[i], partner).wait_send()
    for i in range(len(meta_chip_order)):
        meta_copy(me, meta_chip_send.at[i], partner).wait_send()
    for h in range(2):
        for q in range(4):
            sems = [relay_send.at[h, q, w] for w in range(2)] + [fwd_send.at[h, q, w] for w in range(2)]
            sems += [direct_send.at[h, q, k] for k in range(4)] + [pair_send.at[h, q]]
            for sem in sems:
                rdma(r_buf.at[h, me], rows.at[h, q, 0], sem, rows_recv.at[h, q, 0], partner).wait_send()
        for w in range(2):
            hop1_copy(h, w).wait_send()
            for p in range(2):
                hop2_copy(h, w, p).wait_send()


def solution(mesh):
    num_ep = mesh.shape['ep']
    side = math.isqrt(num_ep // 2)
    assert side == 4 and 2 * side * side == num_ep
    row_spec = P(('dp', 'ep'), None)
    replicated = P()
    expert_spec = P('ep', None, None)
    vmem, anywhere = pl.BlockSpec(memory_space=pltpu.VMEM), pl.BlockSpec(memory_space=pl.ANY)
    dma = pltpu.SemaphoreType.DMA

    def device_step(tokens, expert_ids, gate_vals, slots, shared_w1, shared_w3, shared_w2, shared_gate, expert_w1, expert_w3, expert_w2):
        tok_count, hidden = tokens.shape
        top_k = expert_ids.shape[1]
        local_experts, _, ff = expert_w1.shape
        num_experts = local_experts * num_ep
        capacity = 8 * ((2 * tok_count * top_k + 8 * num_experts - 1) // (8 * num_experts))
        assert local_experts == 2 and top_k < 8 and capacity % 16 == 0 and shared_w1.shape[1] == 2 * ff
        pair = local_experts * capacity
        half = hidden // 2
        y, _, _ = pl.pallas_call(
            functools.partial(layer_kernel, side, capacity),
            out_shape=(jax.ShapeDtypeStruct((tok_count, hidden), BF16),
                       jax.ShapeDtypeStruct((2, num_ep, pair, half), BF16),
                       jax.ShapeDtypeStruct((2, 4, 2, pair, half), BF16)),
            in_specs=[anywhere] + [vmem] * 3 + [anywhere] * 3 + [vmem] + [anywhere] * 3,
            out_specs=(vmem, anywhere, anywhere),
            scratch_shapes=[
                pltpu.VMEM((num_ep, tok_count, hidden), BF16),
                pltpu.VMEM((num_ep, 16, tok_count), F32),
                pltpu.VMEM((2, tok_count, half), F32),
                pltpu.VMEM((local_experts, hidden, ff), BF16),
                pltpu.VMEM((local_experts, hidden, ff), BF16),
                pltpu.VMEM((local_experts, ff, hidden), BF16),
                pltpu.VMEM((2, local_experts, 4 * capacity, hidden), BF16),
                pltpu.VMEM((2, 4, 2 * side, pair, half), BF16),
                pltpu.VMEM((3, 2 * side * pair, tok_count), BF16),
                pltpu.VMEM((2, 3, tok_count, half), F32),
                pltpu.VMEM((2, 2, tok_count // 2, half), F32),
                pltpu.VMEM((2, 2, tok_count, half), F32),
                dma((10,)), dma((4, 15)), dma((64,)), dma((num_ep, 4)), dma((4, 15)), dma((16,)), dma((num_ep,)),
                dma((2, 16)),
                dma((2, 4, 4)), dma((2, 4, 2)), dma((2, 4, 2)), dma((2, 4)), dma((2, 4)), dma((2, 4, 2 * side)),
                dma((2, 4, 2)), dma((2, 2)), dma((2, 2)), dma((2, 2, 2)), dma((2, 2, 2)),
            ],
            compiler_params=pltpu.CompilerParams(collective_id=0, has_side_effects=True, vmem_limit_bytes=VMEM_LIMIT),
            name='moe_layer',
        )(tokens, expert_ids.T, slots.T, gate_vals.T, shared_w1, shared_w3, shared_w2, shared_gate.reshape(1, hidden),
          expert_w1, expert_w3, expert_w2)
        return y

    return jax.shard_map(device_step, mesh=mesh, in_specs=(row_spec, row_spec, row_spec, row_spec, replicated, replicated, replicated, replicated, expert_spec, expert_spec, expert_spec), out_specs=row_spec, check_vma=False)
```

```python
import functools
import math

import jax
import jax.numpy as jnp
from jax import lax
from jax.experimental import pallas as pl
from jax.experimental.pallas import tpu as pltpu
from jax.sharding import PartitionSpec as P

MESH = pl.DeviceIdType.MESH
VMEM_LIMIT = 67043328
F32, BF16 = jnp.float32, jnp.bfloat16

DIRS = ((0, 1), (0, -1), (1, 1), (1, -1))


def wrap(v):
    return (v + 1) % 4 - 1


def shift(axis, way, at):
    moved = list(at)
    moved[axis] = wrap(moved[axis] - way)
    return tuple(moved)


def ahead_piece(way):
    return 0 if way > 0 else 1


def plan_gather():
    queues = [[] for _ in DIRS]
    first = []
    for d, (axis, way) in enumerate(DIRS):
        for half in (axis, 1 - axis):
            for p in (ahead_piece(way), 1 - ahead_piece(way)):
                queues[d].append((half, (0, 0), p))
                first.append((d, (half, (0, 0), p)))
    steps = []
    while any(queues):
        moved = [q.pop(0) if q else None for q in queues]
        arrivals = []
        for d, piece in enumerate(moved):
            if piece is None:
                continue
            half, at, p = piece
            axis, way = DIRS[d]
            at = shift(axis, way, at)
            onward = []
            if p == ahead_piece(way) and abs(at[axis]) == 1:
                onward.append(d)
            if axis == half:
                onward += [e for e, (other, _) in enumerate(DIRS) if other != axis]
            for e in onward:
                queues[e].append((half, at, p))
            arrivals.append((d, (half, at, p), onward))
        steps.append(arrivals)
    return first, steps


def plan_units(steps, chips_per_unit=2):
    done = {(0, 0): 0}
    for i, arrivals in enumerate(steps):
        for _, (_, at, _), _ in arrivals:
            done[at] = i + 1
    order = sorted(done, key=lambda at: (done[at], at))
    units = [order[i : i + chips_per_unit] for i in range(0, len(order), chips_per_unit)]
    return units, [max(done[at] for at in unit) for unit in units]


def carries_meta(piece):
    half, _, p = piece
    return half == 0 and p == 0


def place(side):
    me = lax.axis_index('ep')
    chip = me // 2
    return me, lax.rem(chip, side), chip // side, lax.rem(me, 2)


def pick(table, i):
    out = i * 0 + table[0]
    for k in range(1, len(table)):
        out = jnp.where(i == k, table[k], out)
    return out


def silu_gate(a, b):
    return (jax.nn.silu(a) * b).astype(BF16)


def layer_kernel(side, capacity, tok_in, ids_ref, slots_ref, gates_ref, sw1_in, sw3_in, sw2_in, sg_ref, w1_in, w3_in, w2_in,
                 y_out, r_buf, relay,
                 tok, meta, base, w1, w3, w2, xe, rows, wt, part, hop1, hop2,
                 load_sem, link_send, chip_send, meta_send, link_recv, chip_recv, meta_link_recv, meta_chip_recv, out_sem,
                 direct_send, relay_send, rows_recv, relay_recv, hop1_send, hop1_recv, hop2_send, hop2_recv):
    me, x, y, c = place(side)
    first, steps = plan_gather()
    units, ready = plan_units(steps)
    n_steps = len(steps)
    top_k = ids_ref.shape[0]
    n_tok, hidden = tok_in.shape
    half_cols, half_rows = hidden // 2, n_tok // 2
    ff = w1.shape[2]
    pair = 2 * capacity
    here = (x, y)

    def device(at, core=None):
        dx, dy = at
        col, row = lax.rem(x + (dx + side), side), lax.rem(y + (dy + side), side)
        return (row * side + col) * 2 + (c if core is None else core)

    def along(h, a, b, core):
        return device((a, b) if h == 0 else (b, a), core)

    def neighbour(d, core=None):
        axis, way = DIRS[d]
        return device((way, 0) if axis == 0 else (0, way), core)

    def rdma(src, dst, send, arrive, to):
        return pltpu.make_async_remote_copy(src_ref=src, dst_ref=dst, send_sem=send, recv_sem=arrive,
                                            device_id={'ep': to}, device_id_type=MESH)

    partner = me + 1 - 2 * c

    tok_load = pltpu.make_async_copy(tok_in, tok.at[me], load_sem.at[0])
    tok_load.start()
    shared_loads, expert_loads = [], []
    for j in range(2):
        cols = pl.ds(j * ff, ff)
        shared_loads += [pltpu.make_async_copy(sw1_in.at[:, cols], w1.at[j], load_sem.at[1]),
                         pltpu.make_async_copy(sw3_in.at[:, cols], w3.at[j], load_sem.at[2]),
                         pltpu.make_async_copy(sw2_in.at[cols], w2.at[j], load_sem.at[3])]
    for k, (src, dst) in enumerate(((w1_in, w1), (w3_in, w3), (w2_in, w2))):
        expert_loads.append(pltpu.make_async_copy(src, dst, load_sem.at[1 + k]))
    for load in shared_loads:
        load.start()

    barrier = pltpu.get_barrier_semaphore()
    for to in [neighbour(d, core) for d in range(4) for core in range(2)] + [partner]:
        pl.semaphore_signal(barrier, inc=1, device_id={'ep': to}, device_id_type=MESH)
    slot_of = slots_ref[...]
    meta[me, 0:top_k, :] = jnp.where(slot_of >= 0, ids_ref[...] * capacity + slot_of, -1).astype(F32)
    meta[me, 8 : 8 + top_k, :] = gates_ref[...]
    meta[me, top_k:8, :] = jnp.full((8 - top_k, n_tok), -1.0, F32)
    meta[me, 8 + top_k : 16, :] = jnp.zeros((8 - top_k, n_tok), F32)
    tok_load.wait()
    pl.semaphore_wait(barrier, 9)

    def view(half, src, p):
        return tok.at[src, pl.ds(p * half_rows, half_rows), pl.ds(half * half_cols, half_cols)]

    sent_at = {}
    for i, arrivals in enumerate(steps):
        for d, (half, at, p), _ in arrivals:
            sent_at[d, half, shift(DIRS[d][0], -DIRS[d][1], at), p] = i

    def send_link(d, piece):
        half, at, p = piece
        src, i = device(at), sent_at[d, half, at, p]
        rdma(view(half, src, p), view(half, src, p), link_send.at[0], link_recv.at[i], neighbour(d)).start()
        if carries_meta(piece):
            rdma(meta.at[src], meta.at[src], meta_send.at[0], meta_link_recv.at[i], neighbour(d)).start()

    def send_chip(i, piece):
        half, at, p = piece
        src = device(at)
        rdma(view(half, src, p), view(half, src, p), chip_send.at[0], chip_recv.at[i], partner).start()
        if carries_meta(piece):
            rdma(meta.at[src], meta.at[src], meta_send.at[0], meta_chip_recv.at[i], partner).start()

    own_pieces = [(half, (0, 0), p) for half in range(2) for p in range(2)]

    def await_bytes(sem, ref):
        rdma(ref, ref, sem, sem, partner).wait_recv()

    def await_pieces(pieces, sem, meta_sem):
        await_bytes(sem, tok.at[0])
        n = sum(carries_meta(piece) for piece in pieces)
        if n:
            await_bytes(meta_sem, meta.at[pl.ds(0, n)])

    def do_step(i):
        await_pieces([piece for _, piece, _ in steps[i]], link_recv.at[i], meta_link_recv.at[i])
        for d, piece, onward in steps[i]:
            for e in onward:
                send_link(e, piece)
            send_chip(i + 1, piece)

    def await_chip_step(i):
        pieces = own_pieces if i == 0 else [piece for _, piece, _ in steps[i - 1]]
        await_pieces(pieces, chip_recv.at[i], meta_chip_recv.at[i])

    order = (2, 1, -1, 0)

    def entry(h, hops, core):
        return lax.rem(here[h] + (hops + side), side) * 2 + core

    def send_relay(q):
        for h in range(2):
            for w, way in enumerate((1, -1)):
                rdma(r_buf.at[h, along(h, 2, order[q], w)], relay.at[q, h, w], relay_send.at[0],
                     relay_recv.at[q], along(h, way, 0, c)).start()

    def send_direct(q):
        b = order[q]
        for h in range(2):
            mine = entry(h, 0, c)
            for w, way in enumerate((1, -1)):
                for core in range(2):
                    rdma(r_buf.at[h, along(h, way, b, core)], rows.at[h, q, mine], direct_send.at[0],
                         rows_recv.at[h, q], along(h, way, 0, core)).start()
            rdma(r_buf.at[h, along(h, 0, b, 1 - c)], rows.at[h, q, mine], direct_send.at[0], rows_recv.at[h, q],
                 partner).start()
            pltpu.make_async_copy(r_buf.at[h, along(h, 0, b, c)], rows.at[h, q, mine], rows_recv.at[h, q]).start()

    def forward(q):
        await_bytes(relay_recv.at[q], relay.at[q])
        for h in range(2):
            for w, way in enumerate((1, -1)):
                rdma(relay.at[q, h, w], rows.at[h, q, entry(h, -way, c)], relay_send.at[0], rows_recv.at[h, q],
                     along(h, way, 0, w)).start()

    def await_rows(h, q):
        await_bytes(rows_recv.at[h, q], rows.at[h, q])

    def hop1_copy(h, w):
        return rdma(part.at[h, 0, pl.ds(w * half_rows, half_rows)], hop1.at[h, w], hop1_send.at[0], hop1_recv.at[0],
                    along(h, 0, (1, -1)[w], c))

    def hop2_copy(h, w, p):
        piece = pl.ds(p * half_rows, half_rows)
        return rdma(part.at[h, 1 + w, piece], hop2.at[h, w, piece], hop2_send.at[0], hop2_recv.at[0],
                    along(h, 0, (1, -1)[w], c))

    for d, piece in first:
        send_link(d, piece)
    for piece in own_pieces:
        send_chip(0, piece)

    for load in expert_loads:
        load.wait()
    base[...] = jnp.zeros_like(base)

    def shared_piece(j, _):
        rows_in = tok[me]
        a = jnp.dot(rows_in, w1[j], preferred_element_type=F32)
        b = jnp.dot(rows_in, w3[j], preferred_element_type=F32)
        out = jnp.dot(silu_gate(a, b), w2[j], preferred_element_type=F32)
        for h in range(2):
            base[h] += out[:, h * half_cols : (h + 1) * half_cols]
        return 0

    lax.fori_loop(0, 2, shared_piece, 0)
    for load in expert_loads:
        load.start()
    x_f32 = tok[me].astype(F32)
    logit = jnp.sum(x_f32 * sg_ref[...].astype(F32).reshape(1, hidden), axis=1, keepdims=True)
    for h in range(2):
        base[h] = x_f32[:, h * half_cols : (h + 1) * half_cols] + jax.nn.sigmoid(logit) * base[h]
    for load in expert_loads:
        load.wait()

    row_ids = lax.broadcasted_iota(jnp.int32, (pair, n_tok), 0)
    target = (row_ids + me * pair).astype(F32)
    n_src = 4

    def unit_device(u, i):
        dx = pick([unit[i // 2][0] + side for unit in units], u)
        dy = pick([unit[i // 2][1] + side for unit in units], u)
        col, row = lax.rem(x + dx, side), lax.rem(y + dy, side)
        return (row * side + col) * 2 + i % 2

    def out_copies(slot, srcs):
        return [pltpu.make_async_copy(
                    xe.at[slot, j, pl.ds(i * capacity, capacity), pl.ds(h * half_cols, half_cols)],
                    r_buf.at[h, srcs[i], pl.ds(j * capacity, capacity)],
                    out_sem.at[slot])
                for i in range(n_src) for j in range(2) for h in range(2)]

    def await_out(slot):
        pltpu.make_async_copy(r_buf.at[0, pl.ds(0, 2 * side)], rows.at[0, 0], out_sem.at[slot]).wait()

    n_units = len(units)

    def do_unit(u, _):
        done = 0
        for k, after in enumerate(ready):
            lo, hi = done, after
            done = after

            @pl.when(u == k)
            def _(lo=lo, hi=hi, k=k):
                for i in range(lo, hi):
                    do_step(i)
                for i in range(lo + 1 if lo else 0, hi + 1):
                    await_chip_step(i)

        slot = lax.rem(u, 2)
        srcs = [unit_device(u, i) for i in range(n_src)]
        for i in range(n_src):
            codes = meta[srcs[i], 0:8, :]
            hit = codes[0:1, :] == target
            for k in range(1, top_k):
                hit = jnp.logical_or(hit, codes[k : k + 1, :] == target)
            one_hot = jnp.where(hit, 1.0, 0.0).astype(BF16)
            picked = jnp.dot(one_hot, tok[srcs[i]], preferred_element_type=F32).astype(BF16)
            xe[slot, 0, i * capacity : (i + 1) * capacity, :] = picked[:capacity]
            xe[slot, 1, i * capacity : (i + 1) * capacity, :] = picked[capacity:]

        @pl.when(u >= 1)
        def _():
            await_out(1 - slot)

        @pl.when(u == n_units - 3)
        def _():
            send_direct(1)
            send_direct(2)

        def do_expert(j, _):
            a = jnp.dot(xe[slot, j], w1[j], preferred_element_type=F32)
            b = jnp.dot(xe[slot, j], w3[j], preferred_element_type=F32)
            xe[slot, j] = jnp.dot(silu_gate(a, b), w2[j], preferred_element_type=F32).astype(BF16)
            return 0

        lax.fori_loop(0, 2, do_expert, 0)
        for copy in out_copies(slot, srcs):
            copy.start()
        return 0

    lax.fori_loop(0, n_units, do_unit, 0)
    await_out((n_units - 1) % 2)
    send_relay(0)
    send_direct(0)
    send_relay(1)
    send_relay(2)

    def combine(n, _):
        q, h = n // 2, lax.rem(n, 2)

        @pl.when(n == 0)
        def _():
            forward(0)
            forward(1)
            forward(2)
            send_relay(3)

        @pl.when(n == 2)
        def _():
            send_direct(3)

        @pl.when(n == 6)
        def _():
            forward(3)
            await_bytes(hop1_recv.at[0], hop1)
            for hh in range(2):
                for w in range(2):
                    own = pl.ds(w * half_rows, half_rows)
                    part[hh, 1 + w, own] += hop1[hh, w]
                    hop2_copy(hh, w, w).start()

        for k in range(4):
            for hh in range(2):
                @pl.when(n == 2 * k + hh)
                def _(k=k, hh=hh):
                    await_rows(hh, k)
        b = pick([o + side for o in order], q)
        bx, by = lax.rem(x + jnp.where(h == 0, 0, b), side), lax.rem(y + jnp.where(h == 0, b, 0), side)
        dest = (by * side + bx) * 2 + c
        codes = meta[dest, 0:8, :]
        gates = meta[dest, 8:16, :]

        def weights(g, _):
            gx, gy = jnp.where(h == 0, g // 2, x), jnp.where(h == 0, y, g // 2)
            source = (gy * side + gx) * 2 + lax.rem(g, 2)
            goal = (row_ids + source * pair).astype(F32)
            w = jnp.where(codes[0:1, :] == goal, gates[0:1, :], 0.0)
            for k in range(1, top_k):
                w = jnp.where(codes[k : k + 1, :] == goal, gates[k : k + 1, :], w)
            at = pl.ds(pl.multiple_of(g * pair, pair), pair)
            hi = w.astype(BF16)
            w = w - hi.astype(F32)
            mid = w.astype(BF16)
            wt[0, at, :] = hi
            wt[1, at, :] = mid
            wt[2, at, :] = (w - mid.astype(F32)).astype(BF16)
            return 0

        lax.fori_loop(0, 2 * side, weights, 0)
        block = rows[h, q].reshape(2 * side * pair, half_cols)
        dims = (((0,), (0,)), ((), ()))
        total = lax.dot_general(wt[2], block, dims, preferred_element_type=F32)
        total += lax.dot_general(wt[1], block, dims, preferred_element_type=F32)
        total += lax.dot_general(wt[0], block, dims, preferred_element_type=F32)

        @pl.when(q < 3)
        def _():
            part[h, jnp.minimum(q, 2)] = total

        @pl.when(q == 3)
        def _():
            base[h] += total

        for hh in range(2):
            @pl.when(n == hh)
            def _(hh=hh):
                for w in range(2):
                    hop1_copy(hh, w).start()
            for w in range(2):
                @pl.when(n == 2 * (1 + w) + hh)
                def _(hh=hh, w=w):
                    hop2_copy(hh, w, 1 - w).start()
        return 0

    lax.fori_loop(0, 8, combine, 0)
    await_bytes(hop2_recv.at[0], hop2)
    for h in range(2):
        y_out[:, h * half_cols : (h + 1) * half_cols] = (base[h] + (hop2[h, 0] + hop2[h, 1])).astype(BF16)

    def await_sent(sem, ref):
        rdma(ref, ref, sem, sem, partner).wait_send()

    await_sent(link_send.at[0], tok.at[pl.ds(0, n_steps)])
    await_sent(chip_send.at[0], tok.at[pl.ds(0, n_steps + 1)])
    await_sent(meta_send.at[0], meta.at[pl.ds(0, 2 * n_steps + 1)])
    await_sent(direct_send.at[0], r_buf.at[:, pl.ds(0, 20)])
    await_sent(relay_send.at[0], r_buf.at[:, pl.ds(0, 16)])
    await_sent(hop1_send.at[0], hop1)
    await_sent(hop2_send.at[0], hop2)


def solution(mesh):
    num_ep = mesh.shape['ep']
    side = math.isqrt(num_ep // 2)
    assert side == 4 and 2 * side * side == num_ep
    row_spec = P(('dp', 'ep'), None)
    replicated = P()
    expert_spec = P('ep', None, None)
    vmem, anywhere = pl.BlockSpec(memory_space=pltpu.VMEM), pl.BlockSpec(memory_space=pl.ANY)
    dma = pltpu.SemaphoreType.DMA

    def device_step(tokens, expert_ids, gate_vals, slots, shared_w1, shared_w3, shared_w2, shared_gate, expert_w1, expert_w3, expert_w2):
        tok_count, hidden = tokens.shape
        top_k = expert_ids.shape[1]
        local_experts, _, ff = expert_w1.shape
        num_experts = local_experts * num_ep
        capacity = 8 * ((2 * tok_count * top_k + 8 * num_experts - 1) // (8 * num_experts))
        assert local_experts == 2 and top_k < 8 and capacity % 16 == 0 and shared_w1.shape[1] == 2 * ff
        pair = local_experts * capacity
        half = hidden // 2
        y, _, _ = pl.pallas_call(
            functools.partial(layer_kernel, side, capacity),
            out_shape=(jax.ShapeDtypeStruct((tok_count, hidden), BF16),
                       jax.ShapeDtypeStruct((2, num_ep, pair, half), BF16),
                       jax.ShapeDtypeStruct((4, 2, 2, pair, half), BF16)),
            in_specs=[anywhere] + [vmem] * 3 + [anywhere] * 3 + [vmem] + [anywhere] * 3,
            out_specs=(vmem, anywhere, anywhere),
            scratch_shapes=[
                pltpu.VMEM((num_ep, tok_count, hidden), BF16),
                pltpu.VMEM((num_ep, 16, tok_count), F32),
                pltpu.VMEM((2, tok_count, half), F32),
                pltpu.VMEM((local_experts, hidden, ff), BF16),
                pltpu.VMEM((local_experts, hidden, ff), BF16),
                pltpu.VMEM((local_experts, ff, hidden), BF16),
                pltpu.VMEM((2, local_experts, 4 * capacity, hidden), BF16),
                pltpu.VMEM((2, 4, 2 * side, pair, half), BF16),
                pltpu.VMEM((3, 2 * side * pair, tok_count), BF16),
                pltpu.VMEM((2, 3, tok_count, half), F32),
                pltpu.VMEM((2, 2, tok_count // 2, half), F32),
                pltpu.VMEM((2, 2, tok_count, half), F32),
                dma((4,)), dma((1,)), dma((1,)), dma((1,)), dma((15,)), dma((16,)), dma((15,)), dma((16,)), dma((2,)),
                dma((1,)), dma((1,)), dma((2, 4)), dma((4,)), dma((1,)), dma((1,)), dma((1,)), dma((1,)),
            ],
            compiler_params=pltpu.CompilerParams(collective_id=0, has_side_effects=True, vmem_limit_bytes=VMEM_LIMIT),
            name='moe_layer',
        )(tokens, expert_ids.T, slots.T, gate_vals.T, shared_w1, shared_w3, shared_w2, shared_gate,
          expert_w1, expert_w3, expert_w2)
        return y

    return jax.shard_map(device_step, mesh=mesh, in_specs=(row_spec, row_spec, row_spec, row_spec, replicated, replicated, replicated, replicated, expert_spec, expert_spec, expert_spec), out_specs=row_spec, check_vma=False)
```

```python
import functools
import math

import jax
import jax.numpy as jnp
from jax import lax
from jax.experimental import pallas as pl
from jax.experimental.pallas import tpu as pltpu
from jax.sharding import PartitionSpec as P

MESH = pl.DeviceIdType.MESH
VMEM_LIMIT = 67043328
F32, BF16 = jnp.float32, jnp.bfloat16

DIRS = ((0, 1), (0, -1), (1, 1), (1, -1))


def wrap(v):
    return (v + 1) % 4 - 1


def shift(axis, way, at):
    moved = list(at)
    moved[axis] = wrap(moved[axis] - way)
    return tuple(moved)


def plan_gather():
    slots = []
    for kind, g in (('F1w', 0), ('F1a', 0), ('F2', 0), ('Ga', 0), ('F1f', 0), ('F2', -1), ('F2', 1), ('F2', 2), ('Ga', -1),
                    ('Ga', 1), ('Ga', 2), ('Gb', 0), ('Gb', -1), ('Gb', 1), ('Gb', 2)):
        messages = []
        for d, (a, v) in enumerate(DIRS):
            at = [0, 0]
            quarter = (a, v) if kind in ('F1w', 'F1f') else (a, -v) if kind == 'F1a' else (1 - a, -v if kind == 'Ga' else v)
            if kind in ('F1f', 'Gb'):
                at[a] = -v
            if kind in ('F2', 'Ga', 'Gb'):
                at[1 - a] = wrap(g * quarter[1])
            messages.append((d, quarter, tuple(at)))
        slots.append((kind[0] == 'F', messages))
    sends = {-1: (0, 1, 2, 3), 0: (4, 5), 1: (6,), 4: (7, 8, 9), 5: (10, 11), 9: (12, 13), 10: (14,)}
    return slots, sends


def plan_units(slots, chips_per_unit=2):
    done = {(0, 0): 0}
    for i, (_, messages) in enumerate(slots):
        for d, _, at in messages:
            done[shift(*DIRS[d], at)] = i + 1
    order = sorted(done, key=lambda at: (done[at], at))
    units = [order[i : i + chips_per_unit] for i in range(0, len(order), chips_per_unit)]
    return units, [max(done[at] for at in unit) for unit in units]


def is_whole(quarter, at):
    h, w = quarter
    return at[1 - h] in (0, -w)


def carries_meta(quarter, at):
    h, w = quarter
    if w != 1 or at[h] == 0:
        return False
    if at[1 - h] == 0:
        return True
    return h == (1 if abs(at[0]) == 1 and at[1] == 2 else 0)


def place(side):
    me = lax.axis_index('ep')
    chip = me // 2
    return me, lax.rem(chip, side), chip // side, lax.rem(me, 2)


def pick(table, i):
    out = i * 0 + table[0]
    for k in range(1, len(table)):
        out = jnp.where(i == k, table[k], out)
    return out


def silu_gate(a, b):
    return (jax.nn.silu(a) * b).astype(BF16)


def layer_kernel(side, capacity, tok_in, ids_ref, slots_ref, gates_ref, sw1_in, sw3_in, sw2_in, sg_ref, w1_in, w3_in, w2_in,
                 y_out, r_buf, relay,
                 tok, picked_rows, meta, base, w1, w3, w2, xe, rows, wt, part, hop1, hop2,
                 load_sem, link_send, pick_send, chip_send, meta_send, link_recv, chip_recv, meta_link_recv, meta_chip_recv, out_sem,
                 direct_send, relay_send, rows_recv, relay_recv, hop1_send, hop1_recv, hop2_send, hop2_recv):
    me, x, y, c = place(side)
    slots, sends = plan_gather()
    units, ready = plan_units(slots)
    quarters = [(h, w) for h in range(2) for w in (1, -1)]
    top_k = ids_ref.shape[0]
    n_tok, hidden = tok_in.shape
    half_cols, half_rows = hidden // 2, n_tok // 2
    quarter_cols = hidden // 4
    ff = w1.shape[2]
    pair = 2 * capacity
    here = (x, y)

    def device(at, core=None):
        dx, dy = at
        col, row = lax.rem(x + (dx + side), side), lax.rem(y + (dy + side), side)
        return (row * side + col) * 2 + (c if core is None else core)

    def along(h, a, b, core):
        return device((a, b) if h == 0 else (b, a), core)

    def neighbour(d, core=None):
        axis, way = DIRS[d]
        return device((way, 0) if axis == 0 else (0, way), core)

    def rdma(src, dst, send, arrive, to):
        return pltpu.make_async_remote_copy(src_ref=src, dst_ref=dst, send_sem=send, recv_sem=arrive,
                                            device_id={'ep': to}, device_id_type=MESH)

    partner = me + 1 - 2 * c

    tok_load = pltpu.make_async_copy(tok_in, tok.at[me], load_sem.at[0])
    tok_load.start()
    shared_loads, expert_loads = [], []
    for j in range(2):
        cols = pl.ds(j * ff, ff)
        shared_loads += [pltpu.make_async_copy(sw1_in.at[:, cols], w1.at[j], load_sem.at[1]),
                         pltpu.make_async_copy(sw3_in.at[:, cols], w3.at[j], load_sem.at[2]),
                         pltpu.make_async_copy(sw2_in.at[cols], w2.at[j], load_sem.at[3])]
    for k, (src, dst) in enumerate(((w1_in, w1), (w3_in, w3), (w2_in, w2))):
        expert_loads.append(pltpu.make_async_copy(src, dst, load_sem.at[1 + k]))
    for load in shared_loads:
        load.start()

    barrier = pltpu.get_barrier_semaphore()
    for to in [neighbour(d, core) for d in range(4) for core in range(2)] + [partner]:
        pl.semaphore_signal(barrier, inc=1, device_id={'ep': to}, device_id_type=MESH)
    slot_of = slots_ref[...]
    meta[me, 0:top_k, :] = jnp.where(slot_of >= 0, ids_ref[...] * capacity + slot_of, -1).astype(F32)
    meta[me, 8 : 8 + top_k, :] = gates_ref[...]
    meta[me, top_k:8, :] = jnp.full((8 - top_k, n_tok), -1.0, F32)
    meta[me, 8 + top_k : 16, :] = jnp.zeros((8 - top_k, n_tok), F32)
    tok_load.wait()
    pl.semaphore_wait(barrier, 9)

    def columns(quarter):
        return pl.ds(quarters.index(quarter) * quarter_cols, quarter_cols)

    def view(quarter, src):
        return tok.at[src, :, columns(quarter)]

    def one_hot_rows(codes, goal):
        hit = codes[0:1, :] == goal
        for k in range(1, top_k):
            hit = jnp.logical_or(hit, codes[k : k + 1, :] == goal)
        return jnp.where(hit, 1.0, 0.0).astype(BF16)

    chip_ids = lax.broadcasted_iota(jnp.int32, (2 * pair, n_tok), 0)
    picks = [i for i, (whole, _) in enumerate(slots) if not whole]
    group_of = {i: k % 5 for k, i in enumerate(picks)}

    def await_sent(sem, ref):
        rdma(ref, ref, sem, sem, partner).wait_send()

    def await_picks_sent(group):
        await_sent(pick_send.at[group], tok.at[0, pl.ds(0, 2 * pair)])

    def send_slot(i):
        whole, messages = slots[i]
        if not whole:
            if picks.index(i) >= 5:
                await_picks_sent(group_of[i])
            for d, quarter, at in messages:
                src = device(at)
                goal = (chip_ids + neighbour(d, 0) * pair).astype(F32)
                one_hot = one_hot_rows(meta[src, 0:8, :], goal)
                picked = jnp.dot(one_hot, tok[src, :, columns(quarter)], preferred_element_type=F32)
                picked_rows[group_of[i], d] = picked.astype(BF16)
        for d, quarter, at in messages:
            src = device(at)
            if whole:
                rdma(view(quarter, src), view(quarter, src), link_send.at[0], link_recv.at[i], neighbour(d)).start()
            else:
                for core in range(2):
                    rdma(picked_rows.at[group_of[i], d, pl.ds(core * pair, pair)],
                         tok.at[src, pl.ds(0, pair), columns(quarter)], pick_send.at[group_of[i]], link_recv.at[i], neighbour(d, core)).start()
            if carries_meta(quarter, shift(*DIRS[d], at)):
                for core in (None,) if whole else (0, 1):
                    rdma(meta.at[src], meta.at[src], meta_send.at[0], meta_link_recv.at[i], neighbour(d, core)).start()

    def await_bytes(sem, ref):
        rdma(ref, ref, sem, sem, partner).wait_recv()

    def metas(i):
        return sum(carries_meta(quarter, shift(*DIRS[d], at)) for d, quarter, at in slots[i][1])

    def await_slot(i):
        whole, messages = slots[i]
        await_bytes(link_recv.at[i], tok.at[0] if whole else tok.at[0, pl.ds(0, 2 * pair)])
        if metas(i):
            await_bytes(meta_link_recv.at[i], meta.at[pl.ds(0, metas(i) * (1 if whole else 2))])

    def do_slot(i):
        await_slot(i)
        whole, messages = slots[i]
        if whole:
            for d, quarter, at in messages:
                at = shift(*DIRS[d], at)
                src = device(at)
                rdma(view(quarter, src), view(quarter, src), chip_send.at[0], chip_recv.at[i + 1], partner).start()
                if carries_meta(quarter, at):
                    rdma(meta.at[src], meta.at[src], meta_send.at[0], meta_chip_recv.at[i + 1], partner).start()
        for j in sends.get(i, ()):
            send_slot(j)

    def await_chip_slot(i):
        if i and not slots[i - 1][0]:
            return
        await_bytes(chip_recv.at[i], tok.at[0])
        n = metas(i - 1) if i else 1
        if n:
            await_bytes(meta_chip_recv.at[i], meta.at[pl.ds(0, n)])

    order = (2, 1, -1, 0)

    def entry(h, hops, core):
        return lax.rem(here[h] + (hops + side), side) * 2 + core

    def send_relay(q):
        for h in range(2):
            for w, way in enumerate((1, -1)):
                rdma(r_buf.at[h, along(h, 2, order[q], w)], relay.at[q, h, w], relay_send.at[0],
                     relay_recv.at[q], along(h, way, 0, c)).start()

    def send_direct(q):
        b = order[q]
        for h in range(2):
            mine = entry(h, 0, c)
            for w, way in enumerate((1, -1)):
                for core in range(2):
                    rdma(r_buf.at[h, along(h, way, b, core)], rows.at[h, q, mine], direct_send.at[0],
                         rows_recv.at[h, q], along(h, way, 0, core)).start()
            rdma(r_buf.at[h, along(h, 0, b, 1 - c)], rows.at[h, q, mine], direct_send.at[0], rows_recv.at[h, q],
                 partner).start()
            pltpu.make_async_copy(r_buf.at[h, along(h, 0, b, c)], rows.at[h, q, mine], rows_recv.at[h, q]).start()

    def forward(q):
        await_bytes(relay_recv.at[q], relay.at[q])
        for h in range(2):
            for w, way in enumerate((1, -1)):
                rdma(relay.at[q, h, w], rows.at[h, q, entry(h, -way, c)], relay_send.at[0], rows_recv.at[h, q],
                     along(h, way, 0, w)).start()

    def await_rows(h, q):
        await_bytes(rows_recv.at[h, q], rows.at[h, q])

    def hop1_copy(h, w):
        return rdma(part.at[h, 0, pl.ds(w * half_rows, half_rows)], hop1.at[h, w], hop1_send.at[0], hop1_recv.at[0],
                    along(h, 0, (1, -1)[w], c))

    def hop2_copy(h, w, p):
        piece = pl.ds(p * half_rows, half_rows)
        return rdma(part.at[h, 1 + w, piece], hop2.at[h, w, piece], hop2_send.at[0], hop2_recv.at[0],
                    along(h, 0, (1, -1)[w], c))

    for j in sends[-1]:
        send_slot(j)
    rdma(tok.at[me], tok.at[me], chip_send.at[0], chip_recv.at[0], partner).start()
    rdma(meta.at[me], meta.at[me], meta_send.at[0], meta_chip_recv.at[0], partner).start()

    for load in expert_loads:
        load.wait()
    base[...] = jnp.zeros_like(base)

    def shared_piece(j, _):
        rows_in = tok[me]
        a = jnp.dot(rows_in, w1[j], preferred_element_type=F32)
        b = jnp.dot(rows_in, w3[j], preferred_element_type=F32)
        out = jnp.dot(silu_gate(a, b), w2[j], preferred_element_type=F32)
        for h in range(2):
            base[h] += out[:, h * half_cols : (h + 1) * half_cols]
        return 0

    lax.fori_loop(0, 2, shared_piece, 0)
    for load in expert_loads:
        load.start()
    x_f32 = tok[me].astype(F32)
    logit = jnp.sum(x_f32 * sg_ref[...].astype(F32).reshape(1, hidden), axis=1, keepdims=True)
    for h in range(2):
        base[h] = x_f32[:, h * half_cols : (h + 1) * half_cols] + jax.nn.sigmoid(logit) * base[h]
    for load in expert_loads:
        load.wait()

    row_ids = lax.broadcasted_iota(jnp.int32, (pair, n_tok), 0)
    target = (row_ids + me * pair).astype(F32)
    n_src = 4

    def unit_device(u, i):
        dx = pick([unit[i // 2][0] + side for unit in units], u)
        dy = pick([unit[i // 2][1] + side for unit in units], u)
        col, row = lax.rem(x + dx, side), lax.rem(y + dy, side)
        return (row * side + col) * 2 + i % 2

    def out_copies(slot, srcs):
        return [pltpu.make_async_copy(
                    xe.at[slot, j, pl.ds(i * capacity, capacity), pl.ds(h * half_cols, half_cols)],
                    r_buf.at[h, srcs[i], pl.ds(j * capacity, capacity)],
                    out_sem.at[slot])
                for i in range(n_src) for j in range(2) for h in range(2)]

    def await_out(slot):
        pltpu.make_async_copy(r_buf.at[0, pl.ds(0, 2 * side)], rows.at[0, 0], out_sem.at[slot]).wait()

    n_units = len(units)

    def do_unit(u, _):
        done = 0
        for k, after in enumerate(ready):
            lo, hi = done, after
            done = after

            @pl.when(u == k)
            def _(lo=lo, hi=hi, k=k):
                for i in range(lo, hi):
                    do_slot(i)
                for i in range(lo + 1 if lo else 0, hi + 1):
                    await_chip_slot(i)

        slot = lax.rem(u, 2)
        srcs = [unit_device(u, i) for i in range(n_src)]
        for i in range(n_src):
            one_hot = one_hot_rows(meta[srcs[i], 0:8, :], target)
            for quarter in quarters:
                cols = columns(quarter)
                whole = pick([int(is_whole(quarter, unit[i // 2])) for unit in units], u)

                @pl.when(whole == 1)
                def _(i=i, cols=cols, one_hot=one_hot):
                    picked = jnp.dot(one_hot, tok[srcs[i], :, cols], preferred_element_type=F32).astype(BF16)
                    xe[slot, 0, i * capacity : (i + 1) * capacity, cols] = picked[:capacity]
                    xe[slot, 1, i * capacity : (i + 1) * capacity, cols] = picked[capacity:]

                @pl.when(whole == 0)
                def _(i=i, cols=cols):
                    xe[slot, 0, i * capacity : (i + 1) * capacity, cols] = tok[srcs[i], 0:capacity, cols]
                    xe[slot, 1, i * capacity : (i + 1) * capacity, cols] = tok[srcs[i], capacity:pair, cols]

        @pl.when(u >= 1)
        def _():
            await_out(1 - slot)

        @pl.when(u == n_units - 3)
        def _():
            send_direct(1)
            send_direct(2)

        def do_expert(j, _):
            a = jnp.dot(xe[slot, j], w1[j], preferred_element_type=F32)
            b = jnp.dot(xe[slot, j], w3[j], preferred_element_type=F32)
            xe[slot, j] = jnp.dot(silu_gate(a, b), w2[j], preferred_element_type=F32).astype(BF16)
            return 0

        lax.fori_loop(0, 2, do_expert, 0)
        for copy in out_copies(slot, srcs):
            copy.start()
        return 0

    lax.fori_loop(0, n_units, do_unit, 0)
    await_out((n_units - 1) % 2)
    send_relay(0)
    send_direct(0)
    send_relay(1)
    send_relay(2)

    def combine(n, _):
        q, h = n // 2, lax.rem(n, 2)

        @pl.when(n == 0)
        def _():
            forward(0)
            forward(1)
            forward(2)
            send_relay(3)

        @pl.when(n == 2)
        def _():
            send_direct(3)

        @pl.when(n == 6)
        def _():
            forward(3)
            await_bytes(hop1_recv.at[0], hop1)
            for hh in range(2):
                for w in range(2):
                    own = pl.ds(w * half_rows, half_rows)
                    part[hh, 1 + w, own] += hop1[hh, w]
                    hop2_copy(hh, w, w).start()

        for k in range(4):
            for hh in range(2):
                @pl.when(n == 2 * k + hh)
                def _(k=k, hh=hh):
                    await_rows(hh, k)
        b = pick([o + side for o in order], q)
        bx, by = lax.rem(x + jnp.where(h == 0, 0, b), side), lax.rem(y + jnp.where(h == 0, b, 0), side)
        dest = (by * side + bx) * 2 + c
        codes = meta[dest, 0:8, :]
        gates = meta[dest, 8:16, :]

        def weights(g, _):
            gx, gy = jnp.where(h == 0, g // 2, x), jnp.where(h == 0, y, g // 2)
            source = (gy * side + gx) * 2 + lax.rem(g, 2)
            goal = (row_ids + source * pair).astype(F32)
            w = jnp.where(codes[0:1, :] == goal, gates[0:1, :], 0.0)
            for k in range(1, top_k):
                w = jnp.where(codes[k : k + 1, :] == goal, gates[k : k + 1, :], w)
            at = pl.ds(pl.multiple_of(g * pair, pair), pair)
            hi = w.astype(BF16)
            w = w - hi.astype(F32)
            mid = w.astype(BF16)
            wt[0, at, :] = hi
            wt[1, at, :] = mid
            wt[2, at, :] = (w - mid.astype(F32)).astype(BF16)
            return 0

        lax.fori_loop(0, 2 * side, weights, 0)
        block = rows[h, q].reshape(2 * side * pair, half_cols)
        dims = (((0,), (0,)), ((), ()))
        total = lax.dot_general(wt[2], block, dims, preferred_element_type=F32)
        total += lax.dot_general(wt[1], block, dims, preferred_element_type=F32)
        total += lax.dot_general(wt[0], block, dims, preferred_element_type=F32)

        @pl.when(q < 3)
        def _():
            part[h, jnp.minimum(q, 2)] = total

        @pl.when(q == 3)
        def _():
            base[h] += total

        for hh in range(2):
            @pl.when(n == hh)
            def _(hh=hh):
                for w in range(2):
                    hop1_copy(hh, w).start()
            for w in range(2):
                @pl.when(n == 2 * (1 + w) + hh)
                def _(hh=hh, w=w):
                    hop2_copy(hh, w, 1 - w).start()
        return 0

    lax.fori_loop(0, 8, combine, 0)
    n_whole = sum(whole for whole, _ in slots)
    await_sent(link_send.at[0], tok.at[pl.ds(0, n_whole)])
    for group in range(5):
        await_picks_sent(group)
    await_sent(chip_send.at[0], tok.at[pl.ds(0, n_whole + 1)])
    await_sent(meta_send.at[0], meta.at[pl.ds(0, 2 * len(slots) + 1)])
    await_bytes(hop2_recv.at[0], hop2)
    for h in range(2):
        tok[me, :, h * half_cols : (h + 1) * half_cols] = (base[h] + (hop2[h, 0] + hop2[h, 1])).astype(BF16)
    result = pltpu.make_async_copy(tok.at[me], y_out, load_sem.at[0])
    result.start()
    await_sent(direct_send.at[0], r_buf.at[:, pl.ds(0, 20)])
    await_sent(relay_send.at[0], r_buf.at[:, pl.ds(0, 16)])
    await_sent(hop1_send.at[0], hop1)
    await_sent(hop2_send.at[0], hop2)
    result.wait()


def solution(mesh):
    num_ep = mesh.shape['ep']
    side = math.isqrt(num_ep // 2)
    assert side == 4 and 2 * side * side == num_ep
    row_spec = P(('dp', 'ep'), None)
    replicated = P()
    expert_spec = P('ep', None, None)
    vmem, anywhere = pl.BlockSpec(memory_space=pltpu.VMEM), pl.BlockSpec(memory_space=pl.ANY)
    dma = pltpu.SemaphoreType.DMA

    def device_step(tokens, expert_ids, gate_vals, slots, shared_w1, shared_w3, shared_w2, shared_gate, expert_w1, expert_w3, expert_w2):
        tok_count, hidden = tokens.shape
        top_k = expert_ids.shape[1]
        local_experts, _, ff = expert_w1.shape
        num_experts = local_experts * num_ep
        capacity = 8 * ((2 * tok_count * top_k + 8 * num_experts - 1) // (8 * num_experts))
        assert local_experts == 2 and top_k < 8 and capacity % 16 == 0 and shared_w1.shape[1] == 2 * ff
        pair = local_experts * capacity
        half = hidden // 2
        y, _, _ = pl.pallas_call(
            functools.partial(layer_kernel, side, capacity),
            out_shape=(jax.ShapeDtypeStruct((tok_count, hidden), BF16),
                       jax.ShapeDtypeStruct((2, num_ep, pair, half), BF16),
                       jax.ShapeDtypeStruct((4, 2, 2, pair, half), BF16)),
            in_specs=[anywhere] + [vmem] * 3 + [anywhere] * 3 + [vmem] + [anywhere] * 3,
            out_specs=(anywhere, anywhere, anywhere),
            scratch_shapes=[
                pltpu.VMEM((num_ep, tok_count, hidden), BF16),
                pltpu.VMEM((5, 4, 2 * pair, hidden // 4), BF16),
                pltpu.VMEM((num_ep, 16, tok_count), F32),
                pltpu.VMEM((2, tok_count, half), F32),
                pltpu.VMEM((local_experts, hidden, ff), BF16),
                pltpu.VMEM((local_experts, hidden, ff), BF16),
                pltpu.VMEM((local_experts, ff, hidden), BF16),
                pltpu.VMEM((2, local_experts, 4 * capacity, hidden), BF16),
                pltpu.VMEM((2, 4, 2 * side, pair, half), BF16),
                pltpu.VMEM((3, 2 * side * pair, tok_count), BF16),
                pltpu.VMEM((2, 3, tok_count, half), F32),
                pltpu.VMEM((2, 2, tok_count // 2, half), F32),
                pltpu.VMEM((2, 2, tok_count, half), F32),
                dma((4,)), dma((1,)), dma((5,)), dma((1,)), dma((1,)), dma((15,)), dma((16,)), dma((15,)), dma((16,)), dma((2,)),
                dma((1,)), dma((1,)), dma((2, 4)), dma((4,)), dma((1,)), dma((1,)), dma((1,)), dma((1,)),
            ],
            compiler_params=pltpu.CompilerParams(collective_id=0, has_side_effects=True, vmem_limit_bytes=VMEM_LIMIT),
            name='moe_layer',
        )(tokens, expert_ids.T, slots.T, gate_vals.T, shared_w1, shared_w3, shared_w2, shared_gate,
          expert_w1, expert_w3, expert_w2)
        return y

    return jax.shard_map(device_step, mesh=mesh, in_specs=(row_spec, row_spec, row_spec, row_spec, replicated, replicated, replicated, replicated, expert_spec, expert_spec, expert_spec), out_specs=row_spec, check_vma=False)
```

```python
import functools
import math

import jax
import jax.numpy as jnp
from jax import lax
from jax.experimental import pallas as pl
from jax.experimental.pallas import tpu as pltpu
from jax.sharding import PartitionSpec as P

MESH = pl.DeviceIdType.MESH
VMEM_LIMIT = 67043328
F32, BF16 = jnp.float32, jnp.bfloat16

DIRS = ((0, 1), (0, -1), (1, 1), (1, -1))


def wrap(v):
    return (v + 1) % 4 - 1


def shift(axis, way, at):
    moved = list(at)
    moved[axis] = wrap(moved[axis] - way)
    return tuple(moved)


TREE = (((1, 0), (0, 0)), ((0, 1), (0, 0)), ((2, 0), (1, 0)), ((0, 2), (0, 1)), ((2, 3), (2, 0)),
        ((0, 3), (0, 0)), ((3, 0), (0, 0)), ((3, 1), (0, 1)), ((1, 1), (0, 1)), ((3, 3), (2, 3)),
        ((1, 3), (1, 0)), ((2, 2), (2, 3)), ((1, 2), (0, 2)), ((2, 1), (2, 0)), ((3, 2), (0, 2)))
SLOT = {chip: i for i, (chip, _) in enumerate(TREE)}
INNER = {parent for _, parent in TREE}


def turn(chip, times):
    for _ in range(times % 4):
        chip = (-chip[1] % 4, chip[0])
    return chip


def node(quarter, at):
    return turn((-at[0] % 4, -at[1] % 4), 4 - quarter)


def is_whole(quarter, at):
    return node(quarter, at) in INNER


def carries_meta(quarter, at):
    return quarter == min(range(4), key=lambda k: (SLOT[node(k, at)], k))


def plan_gather():
    ways = [((way, 0) if axis == 0 else (0, way)) for axis, way in DIRS]
    slots = []
    for chip, parent in TREE:
        step = ((chip[0] - parent[0]) % 4, (chip[1] - parent[1]) % 4)
        messages = []
        for d, way in enumerate(ways):
            quarter = next(k for k in range(4) if turn(step, k) == (way[0] % 4, way[1] % 4))
            at = turn(parent, quarter)
            messages.append((d, quarter, (wrap(-at[0]), wrap(-at[1]))))
        slots.append((chip in INNER, messages))
    sends = {-1: (0, 1), 0: (2,), 1: (3,), 2: (4, 5, 6, 7, 8), 4: (9,), 5: (10,), 6: (11,), 7: (12,), 8: (13,), 9: (14,)}
    return slots, sends


def plan_units(slots, chips_per_unit=2):
    done = {(0, 0): 0}
    for i, (_, messages) in enumerate(slots):
        for d, _, at in messages:
            done[shift(*DIRS[d], at)] = i + 1
    order = sorted(done, key=lambda at: (done[at], at))
    units = [order[i : i + chips_per_unit] for i in range(0, len(order), chips_per_unit)]
    return units, [max(done[at] for at in unit) for unit in units]


def place(side):
    me = lax.axis_index('ep')
    chip = me // 2
    return me, lax.rem(chip, side), chip // side, lax.rem(me, 2)


def pick(table, i):
    out = i * 0 + table[0]
    for k in range(1, len(table)):
        out = jnp.where(i == k, table[k], out)
    return out


def silu_gate(a, b):
    return (jax.nn.silu(a) * b).astype(BF16)


def layer_kernel(side, capacity, tok_in, ids_ref, slots_ref, gates_ref, sw1_in, sw3_in, sw2_in, sg_ref, w1_in, w3_in, w2_in,
                 y_out, r_buf, relay,
                 tok, picked_rows, meta, base, w1, w3, w2, xe, rows, wt, part, hop1, hop2,
                 load_sem, link_send, pick_send, chip_send, meta_send, link_recv, chip_recv, meta_link_recv, meta_chip_recv, out_sem,
                 direct_send, relay_send, rows_recv, relay_recv, hop1_send, hop1_recv, hop2_send, hop2_recv):
    me, x, y, c = place(side)
    slots, sends = plan_gather()
    units, ready = plan_units(slots)
    quarters = range(4)
    top_k = ids_ref.shape[0]
    n_tok, hidden = tok_in.shape
    half_cols, half_rows = hidden // 2, n_tok // 2
    quarter_cols = hidden // 4
    ff = w1.shape[2]
    pair = 2 * capacity
    here = (x, y)

    def device(at, core=None):
        dx, dy = at
        col, row = lax.rem(x + (dx + side), side), lax.rem(y + (dy + side), side)
        return (row * side + col) * 2 + (c if core is None else core)

    def along(h, a, b, core):
        return device((a, b) if h == 0 else (b, a), core)

    def neighbour(d, core=None):
        axis, way = DIRS[d]
        return device((way, 0) if axis == 0 else (0, way), core)

    def rdma(src, dst, send, arrive, to):
        return pltpu.make_async_remote_copy(src_ref=src, dst_ref=dst, send_sem=send, recv_sem=arrive,
                                            device_id={'ep': to}, device_id_type=MESH)

    partner = me + 1 - 2 * c

    tok_load = pltpu.make_async_copy(tok_in, tok.at[me], load_sem.at[0])
    tok_load.start()
    shared_loads, expert_loads = [], []
    for j in range(2):
        cols = pl.ds(j * ff, ff)
        shared_loads += [pltpu.make_async_copy(sw1_in.at[:, cols], w1.at[j], load_sem.at[1]),
                         pltpu.make_async_copy(sw3_in.at[:, cols], w3.at[j], load_sem.at[2]),
                         pltpu.make_async_copy(sw2_in.at[cols], w2.at[j], load_sem.at[3])]
    for k, (src, dst) in enumerate(((w1_in, w1), (w3_in, w3), (w2_in, w2))):
        expert_loads.append(pltpu.make_async_copy(src, dst, load_sem.at[1 + k]))
    for load in shared_loads:
        load.start()

    barrier = pltpu.get_barrier_semaphore()
    for to in [neighbour(d, core) for d in range(4) for core in range(2)] + [partner]:
        pl.semaphore_signal(barrier, inc=1, device_id={'ep': to}, device_id_type=MESH)
    slot_of = slots_ref[...]
    meta[me, 0:top_k, :] = jnp.where(slot_of >= 0, ids_ref[...] * capacity + slot_of, -1).astype(F32)
    meta[me, 8 : 8 + top_k, :] = gates_ref[...]
    meta[me, top_k:8, :] = jnp.full((8 - top_k, n_tok), -1.0, F32)
    meta[me, 8 + top_k : 16, :] = jnp.zeros((8 - top_k, n_tok), F32)
    tok_load.wait()
    pl.semaphore_wait(barrier, 9)

    def columns(quarter):
        return pl.ds(quarter * quarter_cols, quarter_cols)

    def view(quarter, src):
        return tok.at[src, :, columns(quarter)]

    def one_hot_rows(codes, goal):
        hit = codes[0:1, :] == goal
        for k in range(1, top_k):
            hit = jnp.logical_or(hit, codes[k : k + 1, :] == goal)
        return jnp.where(hit, 1.0, 0.0).astype(BF16)

    chip_ids = lax.broadcasted_iota(jnp.int32, (2 * pair, n_tok), 0)
    picks = [i for i, (whole, _) in enumerate(slots) if not whole]
    group_of = {i: k % 5 for k, i in enumerate(picks)}

    def await_sent(sem, ref):
        rdma(ref, ref, sem, sem, partner).wait_send()

    def await_picks_sent(group):
        await_sent(pick_send.at[group], tok.at[0, pl.ds(0, 2 * pair)])

    def send_slot(i):
        whole, messages = slots[i]
        if not whole:
            if picks.index(i) >= 5:
                await_picks_sent(group_of[i])
            for d, quarter, at in messages:
                src = device(at)
                goal = (chip_ids + neighbour(d, 0) * pair).astype(F32)
                one_hot = one_hot_rows(meta[src, 0:8, :], goal)
                picked = jnp.dot(one_hot, tok[src, :, columns(quarter)], preferred_element_type=F32)
                picked_rows[group_of[i], d] = picked.astype(BF16)
        for d, quarter, at in messages:
            src = device(at)
            if whole:
                rdma(view(quarter, src), view(quarter, src), link_send.at[0], link_recv.at[i], neighbour(d)).start()
            else:
                for core in range(2):
                    rdma(picked_rows.at[group_of[i], d, pl.ds(core * pair, pair)],
                         tok.at[src, pl.ds(0, pair), columns(quarter)], pick_send.at[group_of[i]], link_recv.at[i], neighbour(d, core)).start()
            if carries_meta(quarter, shift(*DIRS[d], at)):
                for core in (None,) if whole else (0, 1):
                    rdma(meta.at[src], meta.at[src], meta_send.at[0], meta_link_recv.at[i], neighbour(d, core)).start()

    def await_bytes(sem, ref):
        rdma(ref, ref, sem, sem, partner).wait_recv()

    def metas(i):
        return sum(carries_meta(quarter, shift(*DIRS[d], at)) for d, quarter, at in slots[i][1])

    def await_slot(i):
        whole, messages = slots[i]
        await_bytes(link_recv.at[i], tok.at[0] if whole else tok.at[0, pl.ds(0, 2 * pair)])
        if metas(i):
            await_bytes(meta_link_recv.at[i], meta.at[pl.ds(0, metas(i) * (1 if whole else 2))])

    def do_slot(i):
        await_slot(i)
        whole, messages = slots[i]
        if whole:
            for d, quarter, at in messages:
                at = shift(*DIRS[d], at)
                src = device(at)
                rdma(view(quarter, src), view(quarter, src), chip_send.at[0], chip_recv.at[i + 1], partner).start()
                if carries_meta(quarter, at):
                    rdma(meta.at[src], meta.at[src], meta_send.at[0], meta_chip_recv.at[i + 1], partner).start()
        for j in sends.get(i, ()):
            send_slot(j)

    def await_chip_slot(i):
        if i and not slots[i - 1][0]:
            return
        await_bytes(chip_recv.at[i], tok.at[0])
        n = metas(i - 1) if i else 1
        if n:
            await_bytes(meta_chip_recv.at[i], meta.at[pl.ds(0, n)])

    order = (2, 1, -1, 0)

    def entry(h, hops, core):
        return lax.rem(here[h] + (hops + side), side) * 2 + core

    def send_relay(q):
        for h in range(2):
            for w, way in enumerate((1, -1)):
                rdma(r_buf.at[h, along(h, 2, order[q], w)], relay.at[q, h, w], relay_send.at[0],
                     relay_recv.at[q], along(h, way, 0, c)).start()

    def send_direct(q):
        b = order[q]
        for h in range(2):
            mine = entry(h, 0, c)
            for w, way in enumerate((1, -1)):
                for core in range(2):
                    rdma(r_buf.at[h, along(h, way, b, core)], rows.at[h, q, mine], direct_send.at[0],
                         rows_recv.at[h, q], along(h, way, 0, core)).start()
            rdma(r_buf.at[h, along(h, 0, b, 1 - c)], rows.at[h, q, mine], direct_send.at[0], rows_recv.at[h, q],
                 partner).start()
            pltpu.make_async_copy(r_buf.at[h, along(h, 0, b, c)], rows.at[h, q, mine], rows_recv.at[h, q]).start()

    def forward(q):
        await_bytes(relay_recv.at[q], relay.at[q])
        for h in range(2):
            for w, way in enumerate((1, -1)):
                rdma(relay.at[q, h, w], rows.at[h, q, entry(h, -way, c)], relay_send.at[0], rows_recv.at[h, q],
                     along(h, way, 0, w)).start()

    def await_rows(h, q):
        await_bytes(rows_recv.at[h, q], rows.at[h, q])

    def hop1_copy(h, w):
        return rdma(part.at[h, 0, pl.ds(w * half_rows, half_rows)], hop1.at[h, w], hop1_send.at[0], hop1_recv.at[0],
                    along(h, 0, (1, -1)[w], c))

    def hop2_copy(h, w, p):
        piece = pl.ds(p * half_rows, half_rows)
        return rdma(part.at[h, 1 + w, piece], hop2.at[h, w, piece], hop2_send.at[0], hop2_recv.at[0],
                    along(h, 0, (1, -1)[w], c))

    for j in sends[-1]:
        send_slot(j)
    rdma(tok.at[me], tok.at[me], chip_send.at[0], chip_recv.at[0], partner).start()
    rdma(meta.at[me], meta.at[me], meta_send.at[0], meta_chip_recv.at[0], partner).start()

    for load in expert_loads:
        load.wait()
    base[...] = jnp.zeros_like(base)

    def shared_piece(j, _):
        rows_in = tok[me]
        a = jnp.dot(rows_in, w1[j], preferred_element_type=F32)
        b = jnp.dot(rows_in, w3[j], preferred_element_type=F32)
        out = jnp.dot(silu_gate(a, b), w2[j], preferred_element_type=F32)
        for h in range(2):
            base[h] += out[:, h * half_cols : (h + 1) * half_cols]
        return 0

    lax.fori_loop(0, 2, shared_piece, 0)
    for load in expert_loads:
        load.start()
    x_f32 = tok[me].astype(F32)
    logit = jnp.sum(x_f32 * sg_ref[...].astype(F32).reshape(1, hidden), axis=1, keepdims=True)
    for h in range(2):
        base[h] = x_f32[:, h * half_cols : (h + 1) * half_cols] + jax.nn.sigmoid(logit) * base[h]
    for load in expert_loads:
        load.wait()

    row_ids = lax.broadcasted_iota(jnp.int32, (pair, n_tok), 0)
    target = (row_ids + me * pair).astype(F32)
    n_src = 4

    def unit_device(u, i):
        dx = pick([unit[i // 2][0] + side for unit in units], u)
        dy = pick([unit[i // 2][1] + side for unit in units], u)
        col, row = lax.rem(x + dx, side), lax.rem(y + dy, side)
        return (row * side + col) * 2 + i % 2

    def out_copies(slot, srcs):
        return [pltpu.make_async_copy(
                    xe.at[slot, j, pl.ds(i * capacity, capacity), pl.ds(h * half_cols, half_cols)],
                    r_buf.at[h, srcs[i], pl.ds(j * capacity, capacity)],
                    out_sem.at[slot])
                for i in range(n_src) for j in range(2) for h in range(2)]

    def await_out(slot):
        pltpu.make_async_copy(r_buf.at[0, pl.ds(0, 2 * side)], rows.at[0, 0], out_sem.at[slot]).wait()

    n_units = len(units)
    n_early = 1 + max(k for k, unit in enumerate(units) for at in unit if max(at) < 2)
    assert n_early < n_units and max(sends) < ready[n_early - 1]

    def do_unit(u, _):
        done = 0
        for k, after in enumerate(ready):
            lo, hi = done, after
            done = after

            @pl.when(u == k)
            def _(lo=lo, hi=hi, k=k):
                if k == n_early:
                    await_out((k - 1) % 2)
                    send_direct(1)
                    send_direct(2)
                for i in range(lo, hi):
                    do_slot(i)
                for i in range(lo + 1 if lo else 0, hi + 1):
                    await_chip_slot(i)

        slot = lax.rem(u, 2)
        srcs = [unit_device(u, i) for i in range(n_src)]
        for i in range(n_src):
            one_hot = one_hot_rows(meta[srcs[i], 0:8, :], target)
            for quarter in quarters:
                cols = columns(quarter)
                whole = pick([int(is_whole(quarter, unit[i // 2])) for unit in units], u)

                @pl.when(whole == 1)
                def _(i=i, cols=cols, one_hot=one_hot):
                    picked = jnp.dot(one_hot, tok[srcs[i], :, cols], preferred_element_type=F32).astype(BF16)
                    xe[slot, 0, i * capacity : (i + 1) * capacity, cols] = picked[:capacity]
                    xe[slot, 1, i * capacity : (i + 1) * capacity, cols] = picked[capacity:]

                @pl.when(whole == 0)
                def _(i=i, cols=cols):
                    xe[slot, 0, i * capacity : (i + 1) * capacity, cols] = tok[srcs[i], 0:capacity, cols]
                    xe[slot, 1, i * capacity : (i + 1) * capacity, cols] = tok[srcs[i], capacity:pair, cols]

        @pl.when(jnp.logical_and(u >= 1, u != n_early))
        def _():
            await_out(1 - slot)

        def do_expert(j, _):
            a = jnp.dot(xe[slot, j], w1[j], preferred_element_type=F32)
            b = jnp.dot(xe[slot, j], w3[j], preferred_element_type=F32)
            xe[slot, j] = jnp.dot(silu_gate(a, b), w2[j], preferred_element_type=F32).astype(BF16)
            return 0

        lax.fori_loop(0, 2, do_expert, 0)
        for copy in out_copies(slot, srcs):
            copy.start()
        return 0

    lax.fori_loop(0, n_units, do_unit, 0)
    await_out((n_units - 1) % 2)
    send_relay(0)
    send_direct(0)
    send_relay(1)
    send_relay(2)

    def combine(n, _):
        q, h = n // 2, lax.rem(n, 2)

        @pl.when(n == 0)
        def _():
            forward(0)
            forward(1)
            forward(2)
            send_relay(3)

        @pl.when(n == 2)
        def _():
            send_direct(3)

        @pl.when(n == 6)
        def _():
            forward(3)
            await_bytes(hop1_recv.at[0], hop1)
            for hh in range(2):
                for w in range(2):
                    own = pl.ds(w * half_rows, half_rows)
                    part[hh, 1 + w, own] += hop1[hh, w]
                    hop2_copy(hh, w, w).start()

        for k in range(4):
            for hh in range(2):
                @pl.when(n == 2 * k + hh)
                def _(k=k, hh=hh):
                    await_rows(hh, k)
        b = pick([o + side for o in order], q)
        bx, by = lax.rem(x + jnp.where(h == 0, 0, b), side), lax.rem(y + jnp.where(h == 0, b, 0), side)
        dest = (by * side + bx) * 2 + c
        codes = meta[dest, 0:8, :]
        gates = meta[dest, 8:16, :]

        def weights(g, _):
            gx, gy = jnp.where(h == 0, g // 2, x), jnp.where(h == 0, y, g // 2)
            source = (gy * side + gx) * 2 + lax.rem(g, 2)
            goal = (row_ids + source * pair).astype(F32)
            w = jnp.where(codes[0:1, :] == goal, gates[0:1, :], 0.0)
            for k in range(1, top_k):
                w = jnp.where(codes[k : k + 1, :] == goal, gates[k : k + 1, :], w)
            at = pl.ds(pl.multiple_of(g * pair, pair), pair)
            hi = w.astype(BF16)
            w = w - hi.astype(F32)
            mid = w.astype(BF16)
            wt[0, at, :] = hi
            wt[1, at, :] = mid
            wt[2, at, :] = (w - mid.astype(F32)).astype(BF16)
            return 0

        lax.fori_loop(0, 2 * side, weights, 0)
        block = rows[h, q].reshape(2 * side * pair, half_cols)
        dims = (((0,), (0,)), ((), ()))
        total = lax.dot_general(wt[2], block, dims, preferred_element_type=F32)
        total += lax.dot_general(wt[1], block, dims, preferred_element_type=F32)
        total += lax.dot_general(wt[0], block, dims, preferred_element_type=F32)

        @pl.when(q < 3)
        def _():
            part[h, jnp.minimum(q, 2)] = total

        @pl.when(q == 3)
        def _():
            base[h] += total

        for hh in range(2):
            @pl.when(n == hh)
            def _(hh=hh):
                for w in range(2):
                    hop1_copy(hh, w).start()
            for w in range(2):
                @pl.when(n == 2 * (1 + w) + hh)
                def _(hh=hh, w=w):
                    hop2_copy(hh, w, 1 - w).start()
        return 0

    lax.fori_loop(0, 8, combine, 0)
    n_whole = sum(whole for whole, _ in slots)
    await_sent(link_send.at[0], tok.at[pl.ds(0, n_whole)])
    for group in range(5):
        await_picks_sent(group)
    await_sent(chip_send.at[0], tok.at[pl.ds(0, n_whole + 1)])
    await_sent(meta_send.at[0], meta.at[pl.ds(0, 2 * len(slots) + 1)])
    await_bytes(hop2_recv.at[0], hop2)
    for h in range(2):
        tok[me, :, h * half_cols : (h + 1) * half_cols] = (base[h] + (hop2[h, 0] + hop2[h, 1])).astype(BF16)
    result = pltpu.make_async_copy(tok.at[me], y_out, load_sem.at[0])
    result.start()
    await_sent(direct_send.at[0], r_buf.at[:, pl.ds(0, 20)])
    await_sent(relay_send.at[0], r_buf.at[:, pl.ds(0, 16)])
    await_sent(hop1_send.at[0], hop1)
    await_sent(hop2_send.at[0], hop2)
    result.wait()


def solution(mesh):
    num_ep = mesh.shape['ep']
    side = math.isqrt(num_ep // 2)
    assert side == 4 and 2 * side * side == num_ep
    row_spec = P(('dp', 'ep'), None)
    replicated = P()
    expert_spec = P('ep', None, None)
    vmem, anywhere = pl.BlockSpec(memory_space=pltpu.VMEM), pl.BlockSpec(memory_space=pl.ANY)
    dma = pltpu.SemaphoreType.DMA

    def device_step(tokens, expert_ids, gate_vals, slots, shared_w1, shared_w3, shared_w2, shared_gate, expert_w1, expert_w3, expert_w2):
        tok_count, hidden = tokens.shape
        top_k = expert_ids.shape[1]
        local_experts, _, ff = expert_w1.shape
        num_experts = local_experts * num_ep
        capacity = 8 * ((2 * tok_count * top_k + 8 * num_experts - 1) // (8 * num_experts))
        assert local_experts == 2 and top_k < 8 and capacity % 16 == 0 and shared_w1.shape[1] == 2 * ff
        pair = local_experts * capacity
        half = hidden // 2
        y, _, _ = pl.pallas_call(
            functools.partial(layer_kernel, side, capacity),
            out_shape=(jax.ShapeDtypeStruct((tok_count, hidden), BF16),
                       jax.ShapeDtypeStruct((2, num_ep, pair, half), BF16),
                       jax.ShapeDtypeStruct((4, 2, 2, pair, half), BF16)),
            in_specs=[anywhere] + [vmem] * 3 + [anywhere] * 3 + [vmem] + [anywhere] * 3,
            out_specs=(anywhere, anywhere, anywhere),
            scratch_shapes=[
                pltpu.VMEM((num_ep, tok_count, hidden), BF16),
                pltpu.VMEM((5, 4, 2 * pair, hidden // 4), BF16),
                pltpu.VMEM((num_ep, 16, tok_count), F32),
                pltpu.VMEM((2, tok_count, half), F32),
                pltpu.VMEM((local_experts, hidden, ff), BF16),
                pltpu.VMEM((local_experts, hidden, ff), BF16),
                pltpu.VMEM((local_experts, ff, hidden), BF16),
                pltpu.VMEM((2, local_experts, 4 * capacity, hidden), BF16),
                pltpu.VMEM((2, 4, 2 * side, pair, half), BF16),
                pltpu.VMEM((3, 2 * side * pair, tok_count), BF16),
                pltpu.VMEM((2, 3, tok_count, half), F32),
                pltpu.VMEM((2, 2, tok_count // 2, half), F32),
                pltpu.VMEM((2, 2, tok_count, half), F32),
                dma((4,)), dma((1,)), dma((5,)), dma((1,)), dma((1,)), dma((15,)), dma((16,)), dma((15,)), dma((16,)), dma((2,)),
                dma((1,)), dma((1,)), dma((2, 4)), dma((4,)), dma((1,)), dma((1,)), dma((1,)), dma((1,)),
            ],
            compiler_params=pltpu.CompilerParams(collective_id=0, has_side_effects=True, vmem_limit_bytes=VMEM_LIMIT),
            name='moe_layer',
        )(tokens, expert_ids.T, slots.T, gate_vals.T, shared_w1, shared_w3, shared_w2, shared_gate,
          expert_w1, expert_w3, expert_w2)
        return y

    return jax.shard_map(device_step, mesh=mesh, in_specs=(row_spec, row_spec, row_spec, row_spec, replicated, replicated, replicated, replicated, expert_spec, expert_spec, expert_spec), out_specs=row_spec, check_vma=False)
```

```python
import functools
import math

import jax
import jax.numpy as jnp
from jax import lax
from jax.experimental import pallas as pl
from jax.experimental.pallas import tpu as pltpu
from jax.sharding import PartitionSpec as P

MESH = pl.DeviceIdType.MESH
VMEM_LIMIT = 67043328
F32, BF16 = jnp.float32, jnp.bfloat16

DIRS = ((0, 1), (0, -1), (1, 1), (1, -1))


def wrap(v):
    return (v + 1) % 4 - 1


def shift(axis, way, at):
    moved = list(at)
    moved[axis] = wrap(moved[axis] - way)
    return tuple(moved)


TREE = (((1, 0), (0, 0)), ((0, 1), (0, 0)), ((2, 0), (1, 0)), ((0, 2), (0, 1)), ((2, 3), (2, 0)),
        ((0, 3), (0, 0)), ((3, 0), (0, 0)), ((3, 1), (0, 1)), ((1, 1), (0, 1)), ((3, 3), (2, 3)),
        ((1, 3), (1, 0)), ((2, 2), (2, 3)), ((1, 2), (0, 2)), ((2, 1), (2, 0)), ((3, 2), (0, 2)))
SLOT = {chip: i for i, (chip, _) in enumerate(TREE)}
INNER = {parent for _, parent in TREE}


def turn(chip, times):
    for _ in range(times % 4):
        chip = (-chip[1] % 4, chip[0])
    return chip


def node(quarter, at):
    return turn((-at[0] % 4, -at[1] % 4), 4 - quarter)


def is_whole(quarter, at):
    return node(quarter, at) in INNER


def carries_meta(quarter, at):
    return quarter == min(range(4), key=lambda k: (SLOT[node(k, at)], k))


def plan_gather():
    ways = [((way, 0) if axis == 0 else (0, way)) for axis, way in DIRS]
    slots = []
    for chip, parent in TREE:
        step = ((chip[0] - parent[0]) % 4, (chip[1] - parent[1]) % 4)
        messages = []
        for d, way in enumerate(ways):
            quarter = next(k for k in range(4) if turn(step, k) == (way[0] % 4, way[1] % 4))
            at = turn(parent, quarter)
            messages.append((d, quarter, (wrap(-at[0]), wrap(-at[1]))))
        slots.append((chip in INNER, messages))
    sends = {-1: (0, 1), 0: (2,), 1: (3,), 2: (4, 5, 6, 7, 8), 4: (9,), 5: (10,), 6: (11,), 7: (12,), 8: (13,), 9: (14,)}
    return slots, sends


def plan_units(slots, chips_per_unit=2):
    done = {(0, 0): 0}
    for i, (_, messages) in enumerate(slots):
        for d, _, at in messages:
            done[shift(*DIRS[d], at)] = i + 1
    order = sorted(done, key=lambda at: (done[at], at))
    units = [order[i : i + chips_per_unit] for i in range(0, len(order), chips_per_unit)]
    return units, [max(done[at] for at in unit) for unit in units]


def place(side):
    me = lax.axis_index('ep')
    chip = me // 2
    return me, lax.rem(chip, side), chip // side, lax.rem(me, 2)


def pick(table, i):
    out = i * 0 + table[0]
    for k in range(1, len(table)):
        out = jnp.where(i == k, table[k], out)
    return out


def silu_gate(a, b):
    return (jax.nn.silu(a) * b).astype(BF16)


def layer_kernel(side, capacity, tok_in, ids_in, slots_in, gates_in, sw1_in, sw3_in, sw2_in, sg_in, w1_in, w3_in, w2_in,
                 y_out, r_buf, relay,
                 ids_ref, slots_ref, gates_ref, sg_ref, tok, picked_rows, meta, gates, base, w1, w3, w2, xe, rows, wt, part, hop1, hop2,
                 load_sem, link_send, pick_send, chip_send, meta_send, link_recv, chip_recv, meta_link_recv, meta_chip_recv, gates_send, gates_recv, out_sem,
                 direct_send, relay_send, rows_recv, relay_recv, hop1_send, hop1_recv, hop2_send, hop2_recv):
    me, x, y, c = place(side)
    slots, sends = plan_gather()
    units, ready = plan_units(slots)
    quarters = range(4)
    top_k = ids_in.shape[0]
    n_tok, hidden = tok_in.shape
    half_cols, half_rows = hidden // 2, n_tok // 2
    quarter_cols = hidden // 4
    ff = w1.shape[2]
    pair = 2 * capacity
    here = (x, y)

    def device(at, core=None):
        dx, dy = at
        col, row = lax.rem(x + (dx + side), side), lax.rem(y + (dy + side), side)
        return (row * side + col) * 2 + (c if core is None else core)

    def along(h, a, b, core):
        return device((a, b) if h == 0 else (b, a), core)

    def neighbour(d, core=None):
        axis, way = DIRS[d]
        return device((way, 0) if axis == 0 else (0, way), core)

    def rdma(src, dst, send, arrive, to):
        return pltpu.make_async_remote_copy(src_ref=src, dst_ref=dst, send_sem=send, recv_sem=arrive,
                                            device_id={'ep': to}, device_id_type=MESH)

    partner = me + 1 - 2 * c

    barrier = pltpu.get_barrier_semaphore()
    for to in [neighbour(d, core) for d in range(4) for core in range(2)] + [partner]:
        pl.semaphore_signal(barrier, inc=1, device_id={'ep': to}, device_id_type=MESH)
    tok_load = pltpu.make_async_copy(tok_in, tok.at[me], load_sem.at[0])
    small_loads = [pltpu.make_async_copy(src, dst, load_sem.at[4 + k]) for k, (src, dst) in enumerate(
        ((ids_in, ids_ref), (slots_in, slots_ref), (gates_in, gates_ref), (sg_in, sg_ref)))]
    for load in [tok_load] + small_loads:
        load.start()
    shared_loads, expert_loads = [], []
    for j in range(2):
        cols = pl.ds(j * ff, ff)
        shared_loads += [pltpu.make_async_copy(sw1_in.at[:, cols], w1.at[j], load_sem.at[1]),
                         pltpu.make_async_copy(sw3_in.at[:, cols], w3.at[j], load_sem.at[2]),
                         pltpu.make_async_copy(sw2_in.at[cols], w2.at[j], load_sem.at[3])]
    for k, (src, dst) in enumerate(((w1_in, w1), (w3_in, w3), (w2_in, w2))):
        expert_loads.append(pltpu.make_async_copy(src, dst, load_sem.at[1 + k]))
    for load in shared_loads:
        load.start()

    for load in small_loads:
        load.wait()
    slot_of = slots_ref[...]
    meta[me, 0:top_k, :] = jnp.where(slot_of >= 0, ids_ref[...] * capacity + slot_of, -1).astype(F32)
    meta[me, top_k:8, :] = jnp.full((8 - top_k, n_tok), -1.0, F32)
    gates[me, 0:top_k, :] = gates_ref[...]
    gates[me, top_k:8, :] = jnp.zeros((8 - top_k, n_tok), F32)
    tok_load.wait()
    pl.semaphore_wait(barrier, 9)

    def columns(quarter):
        return pl.ds(quarter * quarter_cols, quarter_cols)

    def view(quarter, src):
        return tok.at[src, :, columns(quarter)]

    def one_hot_rows(codes, goal):
        hit = codes[0:1, :] == goal
        for k in range(1, top_k):
            hit = jnp.logical_or(hit, codes[k : k + 1, :] == goal)
        return jnp.where(hit, 1.0, 0.0).astype(BF16)

    chip_ids = lax.broadcasted_iota(jnp.int32, (2 * pair, n_tok), 0)
    picks = [i for i, (whole, _) in enumerate(slots) if not whole]
    group_of = {i: k % 5 for k, i in enumerate(picks)}

    def await_sent(sem, ref):
        rdma(ref, ref, sem, sem, partner).wait_send()

    def await_picks_sent(group):
        await_sent(pick_send.at[group], tok.at[0, pl.ds(0, 2 * pair)])

    def send_slot(i):
        whole, messages = slots[i]
        if not whole:
            if picks.index(i) >= 5:
                await_picks_sent(group_of[i])
            for d, quarter, at in messages:
                src = device(at)
                goal = (chip_ids + neighbour(d, 0) * pair).astype(F32)
                one_hot = one_hot_rows(meta[src, 0:8, :], goal)
                picked = jnp.dot(one_hot, tok[src, :, columns(quarter)], preferred_element_type=F32)
                picked_rows[group_of[i], d] = picked.astype(BF16)
        for d, quarter, at in messages:
            src = device(at)
            if whole:
                rdma(view(quarter, src), view(quarter, src), link_send.at[0], link_recv.at[i], neighbour(d)).start()
            else:
                for core in range(2):
                    rdma(picked_rows.at[group_of[i], d, pl.ds(core * pair, pair)],
                         tok.at[src, pl.ds(0, pair), columns(quarter)], pick_send.at[group_of[i]], link_recv.at[i], neighbour(d, core)).start()
            to_at = shift(*DIRS[d], at)
            if carries_meta(quarter, to_at):
                for core in (None,) if whole else (0, 1):
                    rdma(meta.at[src], meta.at[src], meta_send.at[0], meta_link_recv.at[i], neighbour(d, core)).start()
                if 0 in to_at:
                    assert whole
                    rdma(gates.at[src], gates.at[src], gates_send.at[0], gates_recv.at[i], neighbour(d)).start()

    def await_bytes(sem, ref):
        rdma(ref, ref, sem, sem, partner).wait_recv()

    def metas(i):
        return sum(carries_meta(quarter, shift(*DIRS[d], at)) for d, quarter, at in slots[i][1])

    def await_slot(i):
        whole, messages = slots[i]
        await_bytes(link_recv.at[i], tok.at[0] if whole else tok.at[0, pl.ds(0, 2 * pair)])
        if metas(i):
            await_bytes(meta_link_recv.at[i], meta.at[pl.ds(0, metas(i) * (1 if whole else 2))])
        arrived = [(quarter, shift(*DIRS[d], at)) for d, quarter, at in messages]
        in_line = sum(carries_meta(quarter, at) and 0 in at for quarter, at in arrived)
        if in_line:
            await_bytes(gates_recv.at[i], gates.at[pl.ds(0, in_line)])

    def do_slot(i):
        await_slot(i)
        whole, messages = slots[i]
        if whole:
            for d, quarter, at in messages:
                at = shift(*DIRS[d], at)
                src = device(at)
                rdma(view(quarter, src), view(quarter, src), chip_send.at[0], chip_recv.at[i + 1], partner).start()
                if carries_meta(quarter, at):
                    rdma(meta.at[src], meta.at[src], meta_send.at[0], meta_chip_recv.at[i + 1], partner).start()
        for j in sends.get(i, ()):
            send_slot(j)

    def await_chip_slot(i):
        if i and not slots[i - 1][0]:
            return
        await_bytes(chip_recv.at[i], tok.at[0])
        n = metas(i - 1) if i else 1
        if n:
            await_bytes(meta_chip_recv.at[i], meta.at[pl.ds(0, n)])

    order = (2, 1, -1, 0)

    def entry(h, hops, core):
        return lax.rem(here[h] + (hops + side), side) * 2 + core

    def send_relay(q):
        for h in range(2):
            for w, way in enumerate((1, -1)):
                rdma(r_buf.at[h, along(h, 2, order[q], w)], relay.at[q, h, w], relay_send.at[0],
                     relay_recv.at[q], along(h, way, 0, c)).start()

    def send_direct(q):
        b = order[q]
        for h in range(2):
            mine = entry(h, 0, c)
            for w, way in enumerate((1, -1)):
                for core in range(2):
                    rdma(r_buf.at[h, along(h, way, b, core)], rows.at[h, q, mine], direct_send.at[0],
                         rows_recv.at[h, q], along(h, way, 0, core)).start()
            rdma(r_buf.at[h, along(h, 0, b, 1 - c)], rows.at[h, q, mine], direct_send.at[0], rows_recv.at[h, q],
                 partner).start()
            pltpu.make_async_copy(r_buf.at[h, along(h, 0, b, c)], rows.at[h, q, mine], rows_recv.at[h, q]).start()

    def forward(q):
        await_bytes(relay_recv.at[q], relay.at[q])
        for h in range(2):
            for w, way in enumerate((1, -1)):
                rdma(relay.at[q, h, w], rows.at[h, q, entry(h, -way, c)], relay_send.at[0], rows_recv.at[h, q],
                     along(h, way, 0, w)).start()

    def await_rows(h, q):
        await_bytes(rows_recv.at[h, q], rows.at[h, q])

    def hop1_copy(h, w):
        return rdma(part.at[h, 0, pl.ds(w * half_rows, half_rows)], hop1.at[h, w], hop1_send.at[0], hop1_recv.at[0],
                    along(h, 0, (1, -1)[w], c))

    def hop2_copy(h, w, p):
        piece = pl.ds(p * half_rows, half_rows)
        return rdma(part.at[h, 1 + w, piece], hop2.at[h, w, piece], hop2_send.at[0], hop2_recv.at[0],
                    along(h, 0, (1, -1)[w], c))

    for j in sends[-1]:
        send_slot(j)
    rdma(tok.at[me], tok.at[me], chip_send.at[0], chip_recv.at[0], partner).start()
    rdma(meta.at[me], meta.at[me], meta_send.at[0], meta_chip_recv.at[0], partner).start()

    for load in expert_loads:
        load.wait()
    base[...] = jnp.zeros_like(base)

    def shared_piece(j, _):
        rows_in = tok[me]
        a = jnp.dot(rows_in, w1[j], preferred_element_type=F32)
        b = jnp.dot(rows_in, w3[j], preferred_element_type=F32)
        out = jnp.dot(silu_gate(a, b), w2[j], preferred_element_type=F32)
        for h in range(2):
            base[h] += out[:, h * half_cols : (h + 1) * half_cols]
        return 0

    lax.fori_loop(0, 2, shared_piece, 0)
    for load in expert_loads:
        load.start()
    x_f32 = tok[me].astype(F32)
    logit = jnp.sum(x_f32 * sg_ref[...].astype(F32).reshape(1, hidden), axis=1, keepdims=True)
    for h in range(2):
        base[h] = x_f32[:, h * half_cols : (h + 1) * half_cols] + jax.nn.sigmoid(logit) * base[h]
    for load in expert_loads:
        load.wait()

    row_ids = lax.broadcasted_iota(jnp.int32, (pair, n_tok), 0)
    target = (row_ids + me * pair).astype(F32)
    n_src = 4

    def unit_device(u, i):
        dx = pick([unit[i // 2][0] + side for unit in units], u)
        dy = pick([unit[i // 2][1] + side for unit in units], u)
        col, row = lax.rem(x + dx, side), lax.rem(y + dy, side)
        return (row * side + col) * 2 + i % 2

    def out_copies(slot, srcs):
        return [pltpu.make_async_copy(
                    xe.at[slot, j, pl.ds(i * capacity, capacity), pl.ds(h * half_cols, half_cols)],
                    r_buf.at[h, srcs[i], pl.ds(j * capacity, capacity)],
                    out_sem.at[slot])
                for i in range(n_src) for j in range(2) for h in range(2)]

    def await_out(slot):
        pltpu.make_async_copy(r_buf.at[0, pl.ds(0, 2 * side)], rows.at[0, 0], out_sem.at[slot]).wait()

    n_units = len(units)
    n_early = 1 + max(k for k, unit in enumerate(units) for at in unit if max(at) < 2)
    assert n_early < n_units and max(sends) < ready[n_early - 1]

    def do_unit(u, _):
        done = 0
        for k, after in enumerate(ready):
            lo, hi = done, after
            done = after

            @pl.when(u == k)
            def _(lo=lo, hi=hi, k=k):
                if k == n_early:
                    await_out((k - 1) % 2)
                    send_direct(1)
                    send_direct(2)
                for i in range(lo, hi):
                    do_slot(i)
                for i in range(lo + 1 if lo else 0, hi + 1):
                    await_chip_slot(i)

        slot = lax.rem(u, 2)
        srcs = [unit_device(u, i) for i in range(n_src)]
        for i in range(n_src):
            one_hot = one_hot_rows(meta[srcs[i], 0:8, :], target)
            for quarter in quarters:
                cols = columns(quarter)
                whole = pick([int(is_whole(quarter, unit[i // 2])) for unit in units], u)

                @pl.when(whole == 1)
                def _(i=i, cols=cols, one_hot=one_hot):
                    picked = jnp.dot(one_hot, tok[srcs[i], :, cols], preferred_element_type=F32).astype(BF16)
                    xe[slot, 0, i * capacity : (i + 1) * capacity, cols] = picked[:capacity]
                    xe[slot, 1, i * capacity : (i + 1) * capacity, cols] = picked[capacity:]

                @pl.when(whole == 0)
                def _(i=i, cols=cols):
                    xe[slot, 0, i * capacity : (i + 1) * capacity, cols] = tok[srcs[i], 0:capacity, cols]
                    xe[slot, 1, i * capacity : (i + 1) * capacity, cols] = tok[srcs[i], capacity:pair, cols]

        @pl.when(jnp.logical_and(u >= 1, u != n_early))
        def _():
            await_out(1 - slot)

        def do_expert(j, _):
            a = jnp.dot(xe[slot, j], w1[j], preferred_element_type=F32)
            b = jnp.dot(xe[slot, j], w3[j], preferred_element_type=F32)
            xe[slot, j] = jnp.dot(silu_gate(a, b), w2[j], preferred_element_type=F32).astype(BF16)
            return 0

        lax.fori_loop(0, 2, do_expert, 0)
        for copy in out_copies(slot, srcs):
            copy.start()
        return 0

    lax.fori_loop(0, n_units, do_unit, 0)
    await_out((n_units - 1) % 2)
    send_relay(0)
    send_direct(0)
    send_relay(1)
    send_relay(2)

    def combine(n, _):
        q, h = n // 2, lax.rem(n, 2)

        @pl.when(n == 0)
        def _():
            forward(0)
            forward(1)
            forward(2)
            send_relay(3)

        @pl.when(n == 2)
        def _():
            send_direct(3)

        @pl.when(n == 6)
        def _():
            forward(3)
            await_bytes(hop1_recv.at[0], hop1)
            for hh in range(2):
                for w in range(2):
                    own = pl.ds(w * half_rows, half_rows)
                    part[hh, 1 + w, own] += hop1[hh, w]
                    hop2_copy(hh, w, w).start()

        for k in range(4):
            for hh in range(2):
                @pl.when(n == 2 * k + hh)
                def _(k=k, hh=hh):
                    await_rows(hh, k)
        b = pick([o + side for o in order], q)
        bx, by = lax.rem(x + jnp.where(h == 0, 0, b), side), lax.rem(y + jnp.where(h == 0, b, 0), side)
        dest = (by * side + bx) * 2 + c
        codes = meta[dest, 0:8, :]
        shares = gates[dest]

        def weights(g, _):
            gx, gy = jnp.where(h == 0, g // 2, x), jnp.where(h == 0, y, g // 2)
            source = (gy * side + gx) * 2 + lax.rem(g, 2)
            goal = (row_ids + source * pair).astype(F32)
            w = jnp.where(codes[0:1, :] == goal, shares[0:1, :], 0.0)
            for k in range(1, top_k):
                w = jnp.where(codes[k : k + 1, :] == goal, shares[k : k + 1, :], w)
            at = pl.ds(pl.multiple_of(g * pair, pair), pair)
            hi = w.astype(BF16)
            w = w - hi.astype(F32)
            mid = w.astype(BF16)
            wt[0, at, :] = hi
            wt[1, at, :] = mid
            wt[2, at, :] = (w - mid.astype(F32)).astype(BF16)
            return 0

        lax.fori_loop(0, 2 * side, weights, 0)
        block = rows[h, q].reshape(2 * side * pair, half_cols)
        dims = (((0,), (0,)), ((), ()))
        total = lax.dot_general(wt[2], block, dims, preferred_element_type=F32)
        total += lax.dot_general(wt[1], block, dims, preferred_element_type=F32)
        total += lax.dot_general(wt[0], block, dims, preferred_element_type=F32)

        @pl.when(q < 3)
        def _():
            part[h, jnp.minimum(q, 2)] = total

        @pl.when(q == 3)
        def _():
            base[h] += total

        for hh in range(2):
            @pl.when(n == hh)
            def _(hh=hh):
                for w in range(2):
                    hop1_copy(hh, w).start()
            for w in range(2):
                @pl.when(n == 2 * (1 + w) + hh)
                def _(hh=hh, w=w):
                    hop2_copy(hh, w, 1 - w).start()
        return 0

    lax.fori_loop(0, 8, combine, 0)
    n_whole = sum(whole for whole, _ in slots)
    await_sent(link_send.at[0], tok.at[pl.ds(0, n_whole)])
    for group in range(5):
        await_picks_sent(group)
    await_sent(chip_send.at[0], tok.at[pl.ds(0, n_whole + 1)])
    await_sent(meta_send.at[0], meta.at[pl.ds(0, 2 * len(slots) + 1)])
    await_sent(gates_send.at[0], gates.at[pl.ds(0, 2 * (side - 1))])
    await_bytes(hop2_recv.at[0], hop2)
    results = []
    for p in range(2):
        piece = pl.ds(p * half_rows, half_rows)
        for h in range(2):
            total = base[h, piece] + (hop2[h, 0, piece] + hop2[h, 1, piece])
            tok[me, piece, h * half_cols : (h + 1) * half_cols] = total.astype(BF16)
        results.append(pltpu.make_async_copy(tok.at[me, piece], y_out.at[piece], load_sem.at[p]))
        results[-1].start()
    await_sent(direct_send.at[0], r_buf.at[:, pl.ds(0, 20)])
    await_sent(relay_send.at[0], r_buf.at[:, pl.ds(0, 16)])
    await_sent(hop1_send.at[0], hop1)
    await_sent(hop2_send.at[0], hop2)
    for result in results:
        result.wait()


def solution(mesh):
    num_ep = mesh.shape['ep']
    side = math.isqrt(num_ep // 2)
    assert side == 4 and 2 * side * side == num_ep
    row_spec = P(('dp', 'ep'), None)
    replicated = P()
    expert_spec = P('ep', None, None)
    anywhere = pl.BlockSpec(memory_space=pl.ANY)
    dma = pltpu.SemaphoreType.DMA

    def device_step(tokens, expert_ids, gate_vals, slots, shared_w1, shared_w3, shared_w2, shared_gate, expert_w1, expert_w3, expert_w2):
        tok_count, hidden = tokens.shape
        top_k = expert_ids.shape[1]
        local_experts, _, ff = expert_w1.shape
        num_experts = local_experts * num_ep
        capacity = 8 * ((2 * tok_count * top_k + 8 * num_experts - 1) // (8 * num_experts))
        assert local_experts == 2 and top_k < 8 and capacity % 16 == 0 and shared_w1.shape[1] == 2 * ff
        pair = local_experts * capacity
        half = hidden // 2
        y, _, _ = pl.pallas_call(
            functools.partial(layer_kernel, side, capacity),
            out_shape=(jax.ShapeDtypeStruct((tok_count, hidden), BF16),
                       jax.ShapeDtypeStruct((2, num_ep, pair, half), BF16),
                       jax.ShapeDtypeStruct((4, 2, 2, pair, half), BF16)),
            in_specs=[anywhere] * 11,
            out_specs=(anywhere, anywhere, anywhere),
            scratch_shapes=[
                pltpu.VMEM((top_k, tok_count), jnp.int32),
                pltpu.VMEM((top_k, tok_count), jnp.int32),
                pltpu.VMEM((top_k, tok_count), F32),
                pltpu.VMEM((hidden,), BF16),
                pltpu.VMEM((num_ep, tok_count, hidden), BF16),
                pltpu.VMEM((5, 4, 2 * pair, hidden // 4), BF16),
                pltpu.VMEM((num_ep, 8, tok_count), F32),
                pltpu.VMEM((num_ep, 8, tok_count), F32),
                pltpu.VMEM((2, tok_count, half), F32),
                pltpu.VMEM((local_experts, hidden, ff), BF16),
                pltpu.VMEM((local_experts, hidden, ff), BF16),
                pltpu.VMEM((local_experts, ff, hidden), BF16),
                pltpu.VMEM((2, local_experts, 4 * capacity, hidden), BF16),
                pltpu.VMEM((2, 4, 2 * side, pair, half), BF16),
                pltpu.VMEM((3, 2 * side * pair, tok_count), BF16),
                pltpu.VMEM((2, 3, tok_count, half), F32),
                pltpu.VMEM((2, 2, tok_count // 2, half), F32),
                pltpu.VMEM((2, 2, tok_count, half), F32),
                dma((8,)), dma((1,)), dma((5,)), dma((1,)), dma((1,)), dma((15,)), dma((6,)), dma((15,)), dma((6,)), dma((1,)), dma((3,)), dma((2,)),
                dma((1,)), dma((1,)), dma((2, 4)), dma((4,)), dma((1,)), dma((1,)), dma((1,)), dma((1,)),
            ],
            compiler_params=pltpu.CompilerParams(collective_id=0, has_side_effects=True, vmem_limit_bytes=VMEM_LIMIT),
            name='moe_layer',
        )(tokens, expert_ids.T, slots.T, gate_vals.T, shared_w1, shared_w3, shared_w2, shared_gate,
          expert_w1, expert_w3, expert_w2)
        return y

    return jax.shard_map(device_step, mesh=mesh, in_specs=(row_spec, row_spec, row_spec, row_spec, replicated, replicated, replicated, replicated, expert_spec, expert_spec, expert_spec), out_specs=row_spec, check_vma=False)
```

```python
import functools
import math

import jax
import jax.numpy as jnp
from jax import lax
from jax.experimental import pallas as pl
from jax.experimental.pallas import tpu as pltpu
from jax.sharding import PartitionSpec as P

MESH = pl.DeviceIdType.MESH
VMEM_LIMIT = 67043328
F32, BF16 = jnp.float32, jnp.bfloat16

DIRS = ((0, 1), (0, -1), (1, 1), (1, -1))


def wrap(v):
    return (v + 1) % 4 - 1


def shift(axis, way, at):
    moved = list(at)
    moved[axis] = wrap(moved[axis] - way)
    return tuple(moved)


TREE = (((1, 0), (0, 0)), ((0, 1), (0, 0)), ((2, 0), (1, 0)), ((0, 2), (0, 1)), ((2, 3), (2, 0)),
        ((0, 3), (0, 0)), ((3, 0), (0, 0)), ((3, 1), (0, 1)), ((1, 1), (0, 1)), ((3, 3), (2, 3)),
        ((1, 3), (1, 0)), ((2, 2), (2, 3)), ((1, 2), (0, 2)), ((2, 1), (2, 0)), ((3, 2), (0, 2)))
SLOT = {chip: i for i, (chip, _) in enumerate(TREE)}
INNER = {parent for _, parent in TREE}


def turn(chip, times):
    for _ in range(times % 4):
        chip = (-chip[1] % 4, chip[0])
    return chip


def node(quarter, at):
    return turn((-at[0] % 4, -at[1] % 4), 4 - quarter)


def is_whole(quarter, at):
    return node(quarter, at) in INNER


def carries_meta(quarter, at):
    return quarter == min(range(4), key=lambda k: (SLOT[node(k, at)], k))


def plan_gather():
    ways = [((way, 0) if axis == 0 else (0, way)) for axis, way in DIRS]
    slots = []
    for chip, parent in TREE:
        step = ((chip[0] - parent[0]) % 4, (chip[1] - parent[1]) % 4)
        messages = []
        for d, way in enumerate(ways):
            quarter = next(k for k in range(4) if turn(step, k) == (way[0] % 4, way[1] % 4))
            at = turn(parent, quarter)
            messages.append((d, quarter, (wrap(-at[0]), wrap(-at[1]))))
        slots.append((chip in INNER, messages))
    sends = {-1: (0, 1), 0: (2,), 1: (3,), 2: (4, 5, 6, 7, 8), 4: (9,), 5: (10,), 6: (11,), 7: (12,), 8: (13,), 9: (14,)}
    return slots, sends


def plan_units(slots, chips_per_unit=2):
    done = {(0, 0): 0}
    for i, (_, messages) in enumerate(slots):
        for d, _, at in messages:
            done[shift(*DIRS[d], at)] = i + 1
    order = sorted(done, key=lambda at: (done[at], at))
    units = [order[i : i + chips_per_unit] for i in range(0, len(order), chips_per_unit)]
    return units, [max(done[at] for at in unit) for unit in units]


def place(side):
    me = lax.axis_index('ep')
    chip = me // 2
    return me, lax.rem(chip, side), chip // side, lax.rem(me, 2)


def pick(table, i):
    out = i * 0 + table[0]
    for k in range(1, len(table)):
        out = jnp.where(i == k, table[k], out)
    return out


def silu_gate(a, b):
    return (jax.nn.silu(a) * b).astype(BF16)


def layer_kernel(side, capacity, tok_in, ids_in, slots_in, gates_in, sw1_in, sw3_in, sw2_in, sg_in, w1_in, w3_in, w2_in,
                 y_out, r_buf, relay,
                 ids_ref, slots_ref, gates_ref, sg_ref, tok, picked_rows, meta, gates, base, w1, w3, w2, xe, rows, wt, part, hop1, hop2,
                 load_sem, link_send, pick_send, chip_send, meta_send, link_recv, chip_recv, meta_link_recv, meta_chip_recv, gates_send, gates_recv, out_sem,
                 direct_send, relay_send, rows_recv, relay_recv, hop1_send, hop1_recv, hop2_send, hop2_recv):
    me, x, y, c = place(side)
    slots, sends = plan_gather()
    units, ready = plan_units(slots)
    quarters = range(4)
    top_k = ids_in.shape[0]
    n_tok, hidden = tok_in.shape
    half_cols, half_rows = hidden // 2, n_tok // 2
    quarter_cols = hidden // 4
    ff = w1.shape[2]
    pair = 2 * capacity
    here = (x, y)

    def device(at, core=None):
        dx, dy = at
        col, row = lax.rem(x + (dx + side), side), lax.rem(y + (dy + side), side)
        return (row * side + col) * 2 + (c if core is None else core)

    def along(h, a, b, core):
        return device((a, b) if h == 0 else (b, a), core)

    def neighbour(d, core=None):
        axis, way = DIRS[d]
        return device((way, 0) if axis == 0 else (0, way), core)

    def rdma(src, dst, send, arrive, to):
        return pltpu.make_async_remote_copy(src_ref=src, dst_ref=dst, send_sem=send, recv_sem=arrive,
                                            device_id={'ep': to}, device_id_type=MESH)

    partner = me + 1 - 2 * c

    barrier = pltpu.get_barrier_semaphore()
    for to in [neighbour(d, core) for d in range(4) for core in range(2)] + [partner]:
        pl.semaphore_signal(barrier, inc=1, device_id={'ep': to}, device_id_type=MESH)
    tok_load = pltpu.make_async_copy(tok_in, tok.at[me], load_sem.at[0])
    small_loads = [pltpu.make_async_copy(src, dst, load_sem.at[4 + k]) for k, (src, dst) in enumerate(
        ((ids_in, ids_ref), (slots_in, slots_ref), (gates_in, gates_ref), (sg_in, sg_ref)))]
    for load in [tok_load] + small_loads:
        load.start()
    shared_loads, expert_loads = [], []
    for j in range(2):
        cols = pl.ds(j * ff, ff)
        shared_loads += [pltpu.make_async_copy(sw1_in.at[:, cols], w1.at[j], load_sem.at[1]),
                         pltpu.make_async_copy(sw3_in.at[:, cols], w3.at[j], load_sem.at[2]),
                         pltpu.make_async_copy(sw2_in.at[cols], w2.at[j], load_sem.at[3])]
    for k, (src, dst) in enumerate(((w1_in, w1), (w3_in, w3), (w2_in, w2))):
        expert_loads.append(pltpu.make_async_copy(src, dst, load_sem.at[1 + k]))
    for load in shared_loads:
        load.start()

    for load in small_loads:
        load.wait()
    slot_of = slots_ref[...]
    meta[me, 0:top_k, :] = jnp.where(slot_of >= 0, ids_ref[...] * capacity + slot_of, -1).astype(F32)
    meta[me, top_k:8, :] = jnp.full((8 - top_k, n_tok), -1.0, F32)
    gates[me, 0:top_k, :] = gates_ref[...]
    gates[me, top_k:8, :] = jnp.zeros((8 - top_k, n_tok), F32)
    tok_load.wait()
    pl.semaphore_wait(barrier, 9)

    def columns(quarter):
        return pl.ds(quarter * quarter_cols, quarter_cols)

    def view(quarter, src):
        return tok.at[src, :, columns(quarter)]

    def one_hot_rows(codes, goal):
        hit = codes[0:1, :] == goal
        for k in range(1, top_k):
            hit = jnp.logical_or(hit, codes[k : k + 1, :] == goal)
        return jnp.where(hit, 1.0, 0.0).astype(BF16)

    chip_ids = lax.broadcasted_iota(jnp.int32, (2 * pair, n_tok), 0)
    picks = [i for i, (whole, _) in enumerate(slots) if not whole]
    group_of = {i: k % 5 for k, i in enumerate(picks)}

    def await_sent(sem, ref):
        rdma(ref, ref, sem, sem, partner).wait_send()

    def await_picks_sent(group):
        await_sent(pick_send.at[group], tok.at[0, pl.ds(0, 2 * pair)])

    def send_slot(i):
        whole, messages = slots[i]
        if not whole:
            if picks.index(i) >= 5:
                await_picks_sent(group_of[i])
            for d, quarter, at in messages:
                src = device(at)
                goal = (chip_ids + neighbour(d, 0) * pair).astype(F32)
                one_hot = one_hot_rows(meta[src, 0:8, :], goal)
                picked = jnp.dot(one_hot, tok[src, :, columns(quarter)], preferred_element_type=F32)
                picked_rows[group_of[i], d] = picked.astype(BF16)
        for d, quarter, at in messages:
            src = device(at)
            if whole:
                rdma(view(quarter, src), view(quarter, src), link_send.at[0], link_recv.at[i], neighbour(d)).start()
            else:
                for core in range(2):
                    rdma(picked_rows.at[group_of[i], d, pl.ds(core * pair, pair)],
                         tok.at[src, pl.ds(0, pair), columns(quarter)], pick_send.at[group_of[i]], link_recv.at[i], neighbour(d, core)).start()
            to_at = shift(*DIRS[d], at)
            if carries_meta(quarter, to_at):
                for core in (None,) if whole else (0, 1):
                    rdma(meta.at[src], meta.at[src], meta_send.at[0], meta_link_recv.at[i], neighbour(d, core)).start()
                if 0 in to_at:
                    assert whole
                    rdma(gates.at[src], gates.at[src], gates_send.at[0], gates_recv.at[i], neighbour(d)).start()

    def await_bytes(sem, ref):
        rdma(ref, ref, sem, sem, partner).wait_recv()

    def metas(i):
        return sum(carries_meta(quarter, shift(*DIRS[d], at)) for d, quarter, at in slots[i][1])

    def await_slot(i):
        whole, messages = slots[i]
        await_bytes(link_recv.at[i], tok.at[0] if whole else tok.at[0, pl.ds(0, 2 * pair)])
        if metas(i):
            await_bytes(meta_link_recv.at[i], meta.at[pl.ds(0, metas(i) * (1 if whole else 2))])
        arrived = [(quarter, shift(*DIRS[d], at)) for d, quarter, at in messages]
        in_line = sum(carries_meta(quarter, at) and 0 in at for quarter, at in arrived)
        if in_line:
            await_bytes(gates_recv.at[i], gates.at[pl.ds(0, in_line)])

    def do_slot(i):
        await_slot(i)
        whole, messages = slots[i]
        if whole:
            for d, quarter, at in messages:
                at = shift(*DIRS[d], at)
                src = device(at)
                rdma(view(quarter, src), view(quarter, src), chip_send.at[0], chip_recv.at[i + 1], partner).start()
                if carries_meta(quarter, at):
                    rdma(meta.at[src], meta.at[src], meta_send.at[0], meta_chip_recv.at[i + 1], partner).start()
        for j in sends.get(i, ()):
            send_slot(j)

    def await_chip_slot(i):
        if i and not slots[i - 1][0]:
            return
        await_bytes(chip_recv.at[i], tok.at[0])
        n = metas(i - 1) if i else 1
        if n:
            await_bytes(meta_chip_recv.at[i], meta.at[pl.ds(0, n)])

    order = (2, 1, -1, 0)

    def entry(h, hops, core):
        return lax.rem(here[h] + (hops + side), side) * 2 + core

    def send_relay(q):
        for h in range(2):
            for w, way in enumerate((1, -1)):
                rdma(r_buf.at[h, along(h, 2, order[q], w)], relay.at[q, h, w], relay_send.at[0],
                     relay_recv.at[q], along(h, way, 0, c)).start()

    def send_direct(q):
        b = order[q]
        for h in range(2):
            mine = entry(h, 0, c)
            for w, way in enumerate((1, -1)):
                for core in range(2):
                    rdma(r_buf.at[h, along(h, way, b, core)], rows.at[h, q, mine], direct_send.at[0],
                         rows_recv.at[h, q], along(h, way, 0, core)).start()
            rdma(r_buf.at[h, along(h, 0, b, 1 - c)], rows.at[h, q, mine], direct_send.at[0], rows_recv.at[h, q],
                 partner).start()
            pltpu.make_async_copy(r_buf.at[h, along(h, 0, b, c)], rows.at[h, q, mine], rows_recv.at[h, q]).start()

    def forward(q):
        await_bytes(relay_recv.at[q], relay.at[q])
        for h in range(2):
            for w, way in enumerate((1, -1)):
                rdma(relay.at[q, h, w], rows.at[h, q, entry(h, -way, c)], relay_send.at[0], rows_recv.at[h, q],
                     along(h, way, 0, w)).start()

    def await_rows(h, q):
        await_bytes(rows_recv.at[h, q], rows.at[h, q])

    def hop1_copy(h, w):
        return rdma(part.at[h, 0, pl.ds(w * half_rows, half_rows)], hop1.at[h, w], hop1_send.at[0], hop1_recv.at[0],
                    along(h, 0, (1, -1)[w], c))

    def hop2_copy(h, w, p):
        piece = pl.ds(p * half_rows, half_rows)
        return rdma(part.at[h, 1 + w, piece], hop2.at[h, w, piece], hop2_send.at[0], hop2_recv.at[0],
                    along(h, 0, (1, -1)[w], c))

    for j in sends[-1]:
        send_slot(j)
    rdma(tok.at[me], tok.at[me], chip_send.at[0], chip_recv.at[0], partner).start()
    rdma(meta.at[me], meta.at[me], meta_send.at[0], meta_chip_recv.at[0], partner).start()

    for load in expert_loads:
        load.wait()
    base[...] = jnp.zeros_like(base)

    def shared_piece(j, _):
        rows_in = tok[me]
        a = jnp.dot(rows_in, w1[j], preferred_element_type=F32)
        b = jnp.dot(rows_in, w3[j], preferred_element_type=F32)
        out = jnp.dot(silu_gate(a, b), w2[j], preferred_element_type=F32)
        for h in range(2):
            base[h] += out[:, h * half_cols : (h + 1) * half_cols]
        return 0

    lax.fori_loop(0, 2, shared_piece, 0)
    for load in expert_loads:
        load.start()
    x_f32 = tok[me].astype(F32)
    logit = jnp.sum(x_f32 * sg_ref[...].astype(F32).reshape(1, hidden), axis=1, keepdims=True)
    for h in range(2):
        base[h] = x_f32[:, h * half_cols : (h + 1) * half_cols] + jax.nn.sigmoid(logit) * base[h]
    for load in expert_loads:
        load.wait()

    row_ids = lax.broadcasted_iota(jnp.int32, (pair, n_tok), 0)
    target = (row_ids + me * pair).astype(F32)
    n_src = 4

    def unit_device(u, i):
        dx = pick([unit[i // 2][0] + side for unit in units], u)
        dy = pick([unit[i // 2][1] + side for unit in units], u)
        col, row = lax.rem(x + dx, side), lax.rem(y + dy, side)
        return (row * side + col) * 2 + i % 2

    def out_copies(slot, srcs):
        return [pltpu.make_async_copy(
                    xe.at[slot, j, pl.ds(i * capacity, capacity), pl.ds(h * half_cols, half_cols)],
                    r_buf.at[h, srcs[i], pl.ds(j * capacity, capacity)],
                    out_sem.at[slot])
                for i in range(n_src) for j in range(2) for h in range(2)]

    def await_out(slot):
        pltpu.make_async_copy(r_buf.at[0, pl.ds(0, 2 * side)], rows.at[0, 0], out_sem.at[slot]).wait()

    n_units = len(units)
    n_early = 1 + max(k for k, unit in enumerate(units) for at in unit if max(at) < 2)
    assert n_early < n_units and max(sends) < ready[n_early - 1]

    def do_unit(u, _):
        done = 0
        for k, after in enumerate(ready):
            lo, hi = done, after
            done = after

            @pl.when(u == k)
            def _(lo=lo, hi=hi, k=k):
                if k == n_early:
                    await_out((k - 1) % 2)
                    send_direct(1)
                    send_direct(2)
                for i in range(lo, hi):
                    do_slot(i)
                for i in range(lo + 1 if lo else 0, hi + 1):
                    await_chip_slot(i)

        slot = lax.rem(u, 2)
        srcs = [unit_device(u, i) for i in range(n_src)]
        for i in range(n_src):
            one_hot = one_hot_rows(meta[srcs[i], 0:8, :], target)
            for quarter in quarters:
                cols = columns(quarter)
                whole = pick([int(is_whole(quarter, unit[i // 2])) for unit in units], u)

                @pl.when(whole == 1)
                def _(i=i, cols=cols, one_hot=one_hot):
                    picked = jnp.dot(one_hot, tok[srcs[i], :, cols], preferred_element_type=F32).astype(BF16)
                    xe[slot, 0, i * capacity : (i + 1) * capacity, cols] = picked[:capacity]
                    xe[slot, 1, i * capacity : (i + 1) * capacity, cols] = picked[capacity:]

                @pl.when(whole == 0)
                def _(i=i, cols=cols):
                    xe[slot, 0, i * capacity : (i + 1) * capacity, cols] = tok[srcs[i], 0:capacity, cols]
                    xe[slot, 1, i * capacity : (i + 1) * capacity, cols] = tok[srcs[i], capacity:pair, cols]

        @pl.when(jnp.logical_and(u >= 1, u != n_early))
        def _():
            await_out(1 - slot)

        def do_expert(j, _):
            a = jnp.dot(xe[slot, j], w1[j], preferred_element_type=F32)
            b = jnp.dot(xe[slot, j], w3[j], preferred_element_type=F32)
            xe[slot, j] = jnp.dot(silu_gate(a, b), w2[j], preferred_element_type=F32).astype(BF16)
            return 0

        lax.fori_loop(0, 2, do_expert, 0)
        for copy in out_copies(slot, srcs):
            copy.start()
        return 0

    lax.fori_loop(0, n_units, do_unit, 0)
    await_out((n_units - 1) % 2)
    send_relay(0)
    send_direct(0)
    send_relay(1)
    send_relay(2)

    def combine(n, _):
        q, h = n // 2, lax.rem(n, 2)

        @pl.when(n == 0)
        def _():
            forward(0)
            forward(1)
            forward(2)
            send_relay(3)

        @pl.when(n == 2)
        def _():
            send_direct(3)

        @pl.when(n == 5)
        def _():
            forward(3)

        @pl.when(n == 6)
        def _():
            await_bytes(hop1_recv.at[0], hop1)
            for hh in range(2):
                for w in range(2):
                    own = pl.ds(w * half_rows, half_rows)
                    part[hh, 1 + w, own] += hop1[hh, w]
                    hop2_copy(hh, w, w).start()

        for k in range(4):
            for hh in range(2):
                @pl.when(n == 2 * k + hh)
                def _(k=k, hh=hh):
                    await_rows(hh, k)
        b = pick([o + side for o in order], q)
        bx, by = lax.rem(x + jnp.where(h == 0, 0, b), side), lax.rem(y + jnp.where(h == 0, b, 0), side)
        dest = (by * side + bx) * 2 + c
        codes = meta[dest, 0:8, :]
        shares = gates[dest]

        def weights(g, _):
            gx, gy = jnp.where(h == 0, g // 2, x), jnp.where(h == 0, y, g // 2)
            source = (gy * side + gx) * 2 + lax.rem(g, 2)
            goal = (row_ids + source * pair).astype(F32)
            w = jnp.where(codes[0:1, :] == goal, shares[0:1, :], 0.0)
            for k in range(1, top_k):
                w = jnp.where(codes[k : k + 1, :] == goal, shares[k : k + 1, :], w)
            at = pl.ds(pl.multiple_of(g * pair, pair), pair)
            hi = w.astype(BF16)
            w = w - hi.astype(F32)
            mid = w.astype(BF16)
            wt[0, at, :] = hi
            wt[1, at, :] = mid
            wt[2, at, :] = (w - mid.astype(F32)).astype(BF16)
            return 0

        lax.fori_loop(0, 2 * side, weights, 0)
        block = rows[h, q].reshape(2 * side * pair, half_cols)
        dims = (((0,), (0,)), ((), ()))
        total = lax.dot_general(wt[2], block, dims, preferred_element_type=F32)
        total += lax.dot_general(wt[1], block, dims, preferred_element_type=F32)
        total += lax.dot_general(wt[0], block, dims, preferred_element_type=F32)

        @pl.when(q < 3)
        def _():
            part[h, jnp.minimum(q, 2)] = total

        @pl.when(q == 3)
        def _():
            base[h] += total

        for hh in range(2):
            @pl.when(n == hh)
            def _(hh=hh):
                for w in range(2):
                    hop1_copy(hh, w).start()
            for w in range(2):
                @pl.when(n == 2 * (1 + w) + hh)
                def _(hh=hh, w=w):
                    hop2_copy(hh, w, 1 - w).start()
        return 0

    lax.fori_loop(0, 8, combine, 0)
    n_whole = sum(whole for whole, _ in slots)
    await_sent(link_send.at[0], tok.at[pl.ds(0, n_whole)])
    for group in range(5):
        await_picks_sent(group)
    await_sent(chip_send.at[0], tok.at[pl.ds(0, n_whole + 1)])
    await_sent(meta_send.at[0], meta.at[pl.ds(0, 2 * len(slots) + 1)])
    await_sent(gates_send.at[0], gates.at[pl.ds(0, 2 * (side - 1))])
    await_bytes(hop2_recv.at[0], hop2)
    results = []
    for p in range(2):
        piece = pl.ds(p * half_rows, half_rows)
        for h in range(2):
            total = base[h, piece] + (hop2[h, 0, piece] + hop2[h, 1, piece])
            tok[me, piece, h * half_cols : (h + 1) * half_cols] = total.astype(BF16)
        results.append(pltpu.make_async_copy(tok.at[me, piece], y_out.at[piece], load_sem.at[p]))
        results[-1].start()
    await_sent(direct_send.at[0], r_buf.at[:, pl.ds(0, 20)])
    await_sent(relay_send.at[0], r_buf.at[:, pl.ds(0, 16)])
    await_sent(hop1_send.at[0], hop1)
    await_sent(hop2_send.at[0], hop2)
    for result in results:
        result.wait()


def solution(mesh):
    num_ep = mesh.shape['ep']
    side = math.isqrt(num_ep // 2)
    assert side == 4 and 2 * side * side == num_ep
    row_spec = P(('dp', 'ep'), None)
    replicated = P()
    expert_spec = P('ep', None, None)
    anywhere = pl.BlockSpec(memory_space=pl.ANY)
    dma = pltpu.SemaphoreType.DMA

    def device_step(tokens, expert_ids, gate_vals, slots, shared_w1, shared_w3, shared_w2, shared_gate, expert_w1, expert_w3, expert_w2):
        tok_count, hidden = tokens.shape
        top_k = expert_ids.shape[1]
        local_experts, _, ff = expert_w1.shape
        num_experts = local_experts * num_ep
        capacity = 8 * ((2 * tok_count * top_k + 8 * num_experts - 1) // (8 * num_experts))
        assert local_experts == 2 and top_k < 8 and capacity % 16 == 0 and shared_w1.shape[1] == 2 * ff
        pair = local_experts * capacity
        half = hidden // 2
        y, _, _ = pl.pallas_call(
            functools.partial(layer_kernel, side, capacity),
            out_shape=(jax.ShapeDtypeStruct((tok_count, hidden), BF16),
                       jax.ShapeDtypeStruct((2, num_ep, pair, half), BF16),
                       jax.ShapeDtypeStruct((4, 2, 2, pair, half), BF16)),
            in_specs=[anywhere] * 11,
            out_specs=(anywhere, anywhere, anywhere),
            scratch_shapes=[
                pltpu.VMEM((top_k, tok_count), jnp.int32),
                pltpu.VMEM((top_k, tok_count), jnp.int32),
                pltpu.VMEM((top_k, tok_count), F32),
                pltpu.VMEM((hidden,), BF16),
                pltpu.VMEM((num_ep, tok_count, hidden), BF16),
                pltpu.VMEM((5, 4, 2 * pair, hidden // 4), BF16),
                pltpu.VMEM((num_ep, 8, tok_count), F32),
                pltpu.VMEM((num_ep, 8, tok_count), F32),
                pltpu.VMEM((2, tok_count, half), F32),
                pltpu.VMEM((local_experts, hidden, ff), BF16),
                pltpu.VMEM((local_experts, hidden, ff), BF16),
                pltpu.VMEM((local_experts, ff, hidden), BF16),
                pltpu.VMEM((2, local_experts, 4 * capacity, hidden), BF16),
                pltpu.VMEM((2, 4, 2 * side, pair, half), BF16),
                pltpu.VMEM((3, 2 * side * pair, tok_count), BF16),
                pltpu.VMEM((2, 3, tok_count, half), F32),
                pltpu.VMEM((2, 2, tok_count // 2, half), F32),
                pltpu.VMEM((2, 2, tok_count, half), F32),
                dma((8,)), dma((1,)), dma((5,)), dma((1,)), dma((1,)), dma((15,)), dma((6,)), dma((15,)), dma((6,)), dma((1,)), dma((3,)), dma((2,)),
                dma((1,)), dma((1,)), dma((2, 4)), dma((4,)), dma((1,)), dma((1,)), dma((1,)), dma((1,)),
            ],
            compiler_params=pltpu.CompilerParams(collective_id=0, has_side_effects=True, vmem_limit_bytes=VMEM_LIMIT),
            name='moe_layer',
        )(tokens, expert_ids.T, slots.T, gate_vals.T, shared_w1, shared_w3, shared_w2, shared_gate,
          expert_w1, expert_w3, expert_w2)
        return y

    return jax.shard_map(device_step, mesh=mesh, in_specs=(row_spec, row_spec, row_spec, row_spec, replicated, replicated, replicated, replicated, expert_spec, expert_spec, expert_spec), out_specs=row_spec, check_vma=False)
```
